256 devices in a mesh: dp: 64 (over y, x, z_lo, core), mp: 4 (over z_hi).
Axes of the slice: x: 4, y: 4, z: 8 (z_hi: 4, z_lo: 2; z = z_hi * 2 + z_lo), core: 2. Of those that a mesh axis runs over, the one named last changes fastest.
Arguments:
- feature_ids: int32 [64, 16384, 8], P('dp'), may hold values from 0 to 4095
- tables: bfloat16 [64, 4096, 128], P('dp'), may hold values from -5 to 5
- table_of_feature: int32 [64], replicated, may hold values from 0 to 63, each once
- cross_down: bfloat16 [2, 8192, 512], P(None, 'mp'), may hold values from -0.0625 to 0.0625
- cross_up: bfloat16 [2, 8192, 512], P(None, 'mp'), may hold values from -0.125 to 0.125
- cross_bias: float32 [2, 8192], P(None, 'mp'), may hold values from -3 to 3
- tower_weight: bfloat16 [8192, 2048], P('dp', 'mp'), may hold values from -0.0625 to 0.0625
- tower_bias: float32 [2048], P('mp'), may hold values from -3 to 3
Outputs:
- hidden: bfloat16 [16384, 2048], P('dp', 'mp')
The draws below stay inside these ranges and needn't reach their ends.
Inputs may be any that keep to these rules, and one draw needn't show every extreme that they name: `feature_ids`: each id indexes a row of its own table. `table_of_feature`: each table serves exactly one feature.
All inputs are finite; a program needn't handle non-finite values.
Results may differ from the reference program's by a relative error of at most 0.015.
Values may be sent and summed in bfloat16 or wider, within the bound.
A program may use at most 64 MiB of HBM per device.

```python
import math
import jax
import jax.numpy as jnp
import numpy as np
from jax import lax

EMBED = 128
RANK = 512
HID = 2048
VOCAB = 4096
HOTS = 8
LAYERS = 2
FEATS = 64
WIDTH = 8192
BATCH = 16384


def touch_ends(result, key, smallest, top_value):
    dims = result.shape
    index_at = [jax.random.randint(jax.random.fold_in(key, axis), (), 0, dims[axis]) for axis in range(len(dims))]
    result = result.at[tuple(index_at)].set(smallest)
    longest = dims.index(max(dims))
    index_at[longest] = (index_at[longest] + 1) % dims[longest]
    return result.at[tuple(index_at)].set(top_value)


def block_scale(stream_key, dims, split, least, largest):
    gain = 1.0
    for position, parts in split:
        draws = jax.random.uniform(jax.random.fold_in(jax.random.fold_in(stream_key, 6), position), (parts,), jnp.float32, least / len(split), largest / len(split))
        gain = gain * jnp.repeat(jnp.exp(draws), dims[position] // parts).reshape((-1,) + (1,) * (len(dims) - 1 - position))
    return gain


def cumulative_ranks(number_of, skew):
    portions = [(1 << 20) // math.isqrt(standing ** skew) + 1 for standing in range(1, number_of + 1)]
    width = 1 + sum(portions) // (1 << 30)
    return np.cumsum(np.array([max(1, weight // width) for weight in portions]))


def ranked(key, extent, count, skew):
    table = cumulative_ranks(count, skew)
    pick = jax.random.randint(jax.random.fold_in(key, 1), extent, 0, int(table[count - 1]))
    rank = jnp.searchsorted(jnp.asarray(table, jnp.int32), pick, side="right")
    return jax.random.permutation(jax.random.fold_in(key, 2), count)[rank].astype(jnp.int32)


def centred(key, extent, deviation, limit, shards=(), held_as=jnp.bfloat16):
    loudness = block_scale(key, extent, shards, -0.22, 0.18) if shards else 1.0
    result = jax.random.normal(key, extent, jnp.float32) * deviation * loudness
    return jnp.minimum(jnp.maximum(result, -limit), limit).astype(held_as)


def setup_inputs(seed: int = 0) -> dict:
    key_list = jax.random.split(jax.random.key(seed), 9)
    return {
        "feature_ids": touch_ends(ranked(key_list[0], (FEATS, BATCH, HOTS), VOCAB, 2), jax.random.fold_in(key_list[0], 3), 0, VOCAB - 1).astype(jnp.int32),
        "tables": centred(key_list[1], (FEATS, VOCAB, EMBED), 0.35, 5.0, ((0, 64),)),
        "table_of_feature": jax.random.permutation(key_list[2], FEATS).astype(jnp.int32),
        "cross_down": centred(key_list[3], (LAYERS, WIDTH, RANK), WIDTH ** -0.5, 0.0625, ((1, 4),)),
        "cross_up": centred(key_list[4], (LAYERS, WIDTH, RANK), (4 * RANK) ** -0.5, 0.125, ((1, 4),)),
        "cross_bias": centred(key_list[5], (LAYERS, WIDTH), 0.5, 3.0, ((1, 4),), jnp.float32),
        "tower_weight": centred(key_list[6], (WIDTH, HID), WIDTH ** -0.5, 0.0625, ((0, 64), (1, 4))),
        "tower_bias": centred(key_list[7], (HID,), 0.5, 3.0, ((0, 4),), jnp.float32),
    }


def pool_table(pair):
    table, id_rows = pair
    summed = jnp.zeros((id_rows.shape[0], table.shape[1]), jnp.float32)
    for hot_index in range(HOTS):
        summed = summed + jnp.take(table, id_rows[:, hot_index], axis=0).astype(jnp.float32)
    return summed.astype(jnp.bfloat16)


def reference(feature_ids, tables, table_of_feature, cross_down, cross_up, cross_bias, tower_weight, tower_bias):
    pooled = lax.map(pool_table, (tables, feature_ids))
    ordered = jnp.take(pooled, table_of_feature, axis=0)
    embedded = jnp.transpose(ordered, (1, 0, 2)).reshape(BATCH, WIDTH)
    embedded_wide = embedded.astype(jnp.float32)
    crossed = embedded
    for layer_index in range(LAYERS):
        projected = jnp.dot(crossed, cross_down[layer_index], preferred_element_type=jnp.float32).astype(jnp.bfloat16)
        lifted = lax.dot_general(projected, cross_up[layer_index], (((1,), (1,)), ((), ())), preferred_element_type=jnp.float32)
        crossed = (embedded_wide * (lifted + cross_bias[layer_index]) + crossed.astype(jnp.float32)).astype(jnp.bfloat16)
    pre_act = jnp.dot(crossed, tower_weight, preferred_element_type=jnp.float32) + tower_bias
    return jax.nn.relu(pre_act).astype(jnp.bfloat16)
```

```python
import functools

import jax
import jax.numpy as jnp
from jax import lax
from jax.experimental import pallas as pl
from jax.experimental.pallas import tpu as pltpu
from jax.sharding import PartitionSpec as P

MESH = pl.DeviceIdType.MESH
VMEM = pltpu.VMEM
F32 = jnp.float32
BF16 = jnp.bfloat16
WHOLE = pl.BlockSpec(memory_space=pltpu.VMEM)
SCALARS = pl.BlockSpec(memory_space=pltpu.SMEM)


def pool_kernel(hots, blocks, rows, ids_ref, table_ref, out_ref, wide, acc):
    vocab = table_ref.shape[0]
    samples = blocks * rows
    step = 256

    def widen(i, carry):
        at = pl.ds(pl.multiple_of(i * step, step), step)
        wide[at, :] = table_ref[at, :].astype(F32)
        return carry

    lax.fori_loop(0, vocab // step, widen, 0)

    def block(g, carry):
        def eight(q, carry):
            first = g * rows + q * 8
            for j in range(8):
                total = wide[pl.ds(ids_ref[first + j], 1), :]
                for h in range(1, hots):
                    total = total + wide[pl.ds(ids_ref[h * samples + first + j], 1), :]
                acc[pl.ds(q * 8 + j, 1), :] = total
            return carry

        lax.fori_loop(0, rows // 8, eight, 0)
        out_ref[g] = acc[...].astype(BF16)
        return carry

    lax.fori_loop(0, blocks, block, 0)


def pooled_rows(own_ids, table, hots, blocks, rows):
    vocab, width = table.shape
    return pl.pallas_call(
        functools.partial(pool_kernel, hots, blocks, rows),
        out_shape=jax.ShapeDtypeStruct((blocks, rows, width), BF16),
        in_specs=[SCALARS, WHOLE],
        out_specs=WHOLE,
        scratch_shapes=[VMEM((vocab, width), F32), VMEM((rows, width), F32)],
        name="pool",
        cost_estimate=pl.CostEstimate(flops=40_000_000_000, bytes_accessed=3_000_000, transcendentals=0),
    )(own_ids, table)


def barrier_with(others):
    barrier = pltpu.get_barrier_semaphore()
    count = 0
    for loop, device in others:
        def one(k, carry, device=device):
            pl.semaphore_signal(barrier, inc=1, device_id=device(k), device_id_type=MESH)
            return carry

        lax.fori_loop(1, loop, one, 0)
        count += loop - 1
    pl.semaphore_wait(barrier, count)


def regroup_kernel(groups, members, order_ref, pooled_ref, emb_ref, recv, packed, send_sem, recv_sem, mp_send, mp_recv):
    d = lax.axis_index("dp")
    m = lax.axis_index("mp")
    rows, width = pooled_ref.shape[1:]
    per = groups // members

    def dp_at(k):
        return (lax.rem(d + k, groups), m)

    def mp_at(k):
        return (d, lax.rem(m + k, members))

    barrier_with(((groups, dp_at), (members, mp_at)))

    def dp_copy(k):
        return pltpu.make_async_remote_copy(
            src_ref=pooled_ref.at[lax.rem(d + k, groups)],
            dst_ref=recv.at[d],
            send_sem=send_sem,
            recv_sem=recv_sem,
            device_id=dp_at(k),
            device_id_type=MESH,
        )

    def start(k, carry):
        dp_copy(k).start()
        return carry

    lax.fori_loop(1, groups, start, 0)
    recv[d] = pooled_ref[d]
    every = pltpu.make_async_remote_copy(
        src_ref=pooled_ref.at[pl.ds(0, groups - 1)],
        dst_ref=recv.at[pl.ds(0, groups - 1)],
        send_sem=send_sem,
        recv_sem=recv_sem,
        device_id=dp_at(1),
        device_id_type=MESH,
    )
    every.wait_recv()
    for p in range(groups):
        packed[p // per, :, (p % per) * width : (p % per + 1) * width] = recv[order_ref[p]]
    copies = []
    for k in range(1, members):
        to = lax.rem(m + k, members)
        copies.append(
            pltpu.make_async_remote_copy(
                src_ref=packed.at[to],
                dst_ref=emb_ref.at[m],
                send_sem=mp_send.at[k - 1],
                recv_sem=mp_recv.at[k - 1],
                device_id=mp_at(k),
                device_id_type=MESH,
            )
        )
        copies[-1].start()
    emb_ref[m] = packed[m]
    every.wait_send()
    for copy in copies:
        copy.wait()


def regrouped(pooled, order, groups, members):
    _, rows, width = pooled.shape
    per = groups // members
    return pl.pallas_call(
        functools.partial(regroup_kernel, groups, members),
        out_shape=jax.ShapeDtypeStruct((members, rows, per * width), BF16),
        in_specs=[SCALARS, WHOLE],
        out_specs=WHOLE,
        scratch_shapes=[
            VMEM((groups, rows, width), BF16),
            VMEM((members, rows, per * width), BF16),
            pltpu.SemaphoreType.DMA,
            pltpu.SemaphoreType.DMA,
            pltpu.SemaphoreType.DMA((members - 1,)),
            pltpu.SemaphoreType.DMA((members - 1,)),
        ],
        compiler_params=pltpu.CompilerParams(collective_id=0, has_side_effects=True),
        name="regroup",
        cost_estimate=pl.CostEstimate(flops=40_000_000_000, bytes_accessed=3_000_000, transcendentals=0),
    )(order, pooled)


def cross_kernel(
    members, emb_ref, down_ref, up_ref, bias_ref, tower_ref, tower_bias_ref, out_ref,
    part, arrived, proj, crossed, partial_units, units_in, send_sem, recv_sem,
):
    d = lax.axis_index("dp")
    m = lax.axis_index("mp")
    rows, cols = emb_ref.shape
    layers, _, rank = down_ref.shape
    share = rows // members
    units = out_ref.shape[1]

    def mp_at(k):
        return (d, lax.rem(m + k, members))

    barrier_with(((members, mp_at),))

    def copy_to(k, phase, src, dst):
        return pltpu.make_async_remote_copy(
            src_ref=src,
            dst_ref=dst,
            send_sem=send_sem.at[phase, k - 1],
            recv_sem=recv_sem.at[phase, k - 1],
            device_id=mp_at(k),
            device_id_type=MESH,
        )

    tile = min(512, cols)
    for layer in range(layers):
        source = emb_ref if layer == 0 else crossed
        product = jnp.dot(source[...], down_ref[layer], preferred_element_type=F32)
        part[layer] = product.astype(BF16).reshape(members, share, rank)
        copies = []
        for k in range(1, members):
            to = lax.rem(m + k, members)
            copies.append(copy_to(k, 2 * layer, part.at[layer, to], arrived.at[layer, k - 1]))
            copies[-1].start()
        total = part[layer, m].astype(F32)
        for k in range(1, members):
            copies[k - 1].wait()
            total = total + arrived[layer, k - 1].astype(F32)
        proj[layer, m] = total.astype(BF16)
        copies = []
        for k in range(1, members):
            copies.append(copy_to(k, 2 * layer + 1, proj.at[layer, m], proj.at[layer, m]))
            copies[-1].start()
        for copy in copies:
            copy.wait()
        projected = proj[layer].reshape(rows, rank)

        def columns(i, carry, layer=layer, source=source, projected=projected):
            at = pl.ds(pl.multiple_of(i * tile, tile), tile)
            lifted = lax.dot_general(
                projected, up_ref[layer, at, :], (((1,), (1,)), ((), ())), preferred_element_type=F32
            )
            value = emb_ref[:, at].astype(F32) * (lifted + bias_ref[layer : layer + 1, at])
            crossed[:, at] = (value + source[:, at].astype(F32)).astype(BF16)
            return carry

        lax.fori_loop(0, cols // tile, columns, 0)

    def tower(block):
        at = pl.ds(pl.multiple_of(block * cols, cols), cols)
        return jnp.dot(crossed[...], tower_ref[at, :], preferred_element_type=F32)

    def send_units(k, carry):
        to = lax.rem(m + k, members)
        partial_units[k - 1] = tower(to).astype(BF16)
        copy_to(k, 2 * layers, partial_units.at[k - 1], units_in.at[k - 1]).start()
        return carry

    lax.fori_loop(1, members, send_units, 0)
    total = tower(m) + tower_bias_ref[...]
    for k in range(1, members):
        copy_to(k, 2 * layers, partial_units.at[k - 1], units_in.at[k - 1]).wait()
        total = total + units_in[k - 1].astype(F32)
    out_ref[...] = jnp.maximum(total, 0.0).astype(BF16)


def crossed_and_towered(emb, down, up, bias, tower, tower_bias, members):
    rows, cols = emb.shape
    layers, _, rank = down.shape
    units = tower.shape[1]
    share = rows // members
    phases = 2 * layers + 1
    return pl.pallas_call(
        functools.partial(cross_kernel, members),
        out_shape=jax.ShapeDtypeStruct((rows, units), BF16),
        in_specs=[WHOLE] * 6,
        out_specs=WHOLE,
        scratch_shapes=[
            VMEM((layers, members, share, rank), BF16),
            VMEM((layers, members - 1, share, rank), BF16),
            VMEM((layers, members, share, rank), BF16),
            VMEM((rows, cols), BF16),
            VMEM((members - 1, rows, units), BF16),
            VMEM((members - 1, rows, units), BF16),
            pltpu.SemaphoreType.DMA((phases, members - 1)),
            pltpu.SemaphoreType.DMA((phases, members - 1)),
        ],
        compiler_params=pltpu.CompilerParams(
            collective_id=1, has_side_effects=True, vmem_limit_bytes=48 * 1024 * 1024
        ),
        name="cross",
        cost_estimate=pl.CostEstimate(flops=4_000_000_000, bytes_accessed=20_000_000, transcendentals=0),
    )(emb, down, up, bias, tower, tower_bias)


def body(groups, members, feature_ids, tables, table_of_feature, cross_down, cross_up, cross_bias, tower_weight, tower_bias):
    m = lax.axis_index("mp")
    _, batch, hots = feature_ids.shape
    rows = batch // (groups * members)
    per = groups // members
    swap = []
    for a in range(members):
        for b in range(per):
            for z in range(members):
                swap.append(((a * per + b) * members + z, (z * per + b) * members + a))
    turned = lax.ppermute(tower_weight, ("dp", "mp"), swap)
    tower = lax.all_gather(turned, "dp", axis=0, tiled=True)
    by_hot = jnp.transpose(feature_ids[0]).reshape(hots, groups, members, rows)
    own_ids = lax.dynamic_index_in_dim(by_hot, m, 2, keepdims=False).reshape(-1)
    pooled = pooled_rows(own_ids, tables[0], hots, groups, rows)
    emb = regrouped(pooled, table_of_feature, groups, members)
    emb = emb.reshape(members * rows, -1)
    return crossed_and_towered(
        emb, cross_down, cross_up, cross_bias, tower, tower_bias.reshape(1, -1), members
    )


def solution(mesh):
    groups, members = mesh.shape["dp"], mesh.shape["mp"]
    return jax.shard_map(
        functools.partial(body, groups, members),
        mesh=mesh,
        in_specs=(
            P("dp", None, None),
            P("dp", None, None),
            P(),
            P(None, "mp", None),
            P(None, "mp", None),
            P(None, "mp"),
            P("dp", "mp"),
            P("mp"),
        ),
        out_specs=P("dp", "mp"),
        check_vma=False,
    )
```

```python
import functools

import jax
import jax.numpy as jnp
from jax import lax
from jax.experimental import pallas as pl
from jax.experimental.pallas import tpu as pltpu
from jax.sharding import PartitionSpec as P

MESH = pl.DeviceIdType.MESH
VMEM = pltpu.VMEM
DMA = pltpu.SemaphoreType.DMA
F32 = jnp.float32
BF16 = jnp.bfloat16
WHOLE = pl.BlockSpec(memory_space=pltpu.VMEM)
SCALARS = pl.BlockSpec(memory_space=pltpu.SMEM)
ANY = pl.BlockSpec(memory_space=pl.ANY)
LANES = 128
CHUNKS = 4
GROUPS = 2


def torus(groups, members):
    rest = groups // members
    across = min(4, rest)
    rest //= across
    below = min(2, rest)
    return members, across, below, rest // below


def place(sizes, d):
    _, nx, nz, nc = sizes
    return d // (nx * nz * nc), lax.rem(d // (nz * nc), nx), lax.rem(d // nc, nz), lax.rem(d, nc)


def index_of(sizes, y, x, z, c):
    _, nx, nz, nc = sizes
    return ((y * nx + x) * nz + z) * nc + c


def signal(device):
    pl.semaphore_signal(pltpu.get_barrier_semaphore(), inc=1, device_id=device, device_id_type=MESH)


def remote(src, dst, send, recv, device):
    return pltpu.make_async_remote_copy(
        src_ref=src, dst_ref=dst, send_sem=send, recv_sem=recv, device_id=device, device_id_type=MESH
    )


def regroup_kernel(
    groups, members, hots, ids_hbm, order_ref, table_ref, weight_ref, emb_ref, quarter_ref,
    ids_ref, wide, acc, pooled, recv, packed, mine, ids_sem,
    send_sem, recv_sem, mp_send, mp_recv, w_send, w_recv,
):
    d = lax.axis_index("dp")
    m = lax.axis_index("mp")
    vocab, width = table_ref.shape
    chunk = pooled.shape[2]
    per = groups // members
    sizes = torus(groups, members)
    ny, nx, nz, nc = sizes
    y, x, z, c = place(sizes, d)

    ids_copy = pltpu.make_async_copy(ids_hbm, ids_ref, ids_sem)
    ids_copy.start()

    def dp_at(k):
        return (lax.rem(d + k, groups), m)

    def mp_at(k):
        return (d, lax.rem(m + k, members))

    turned = (m * per + lax.rem(d, per), d // per)
    moved = d // per != m
    for count, device in ((groups, dp_at), (members, mp_at)):

        def greet(k, carry, device=device):
            signal(device(k))
            return carry

        lax.fori_loop(1, count, greet, 0)

    @pl.when(moved)
    def _():
        signal(turned)

    pl.semaphore_wait(
        pltpu.get_barrier_semaphore(), groups + members - 2 + jnp.where(moved, 1, 0).astype(jnp.int32)
    )

    swap = remote(weight_ref, mine, w_send.at[0], w_recv.at[0], turned)

    @pl.when(moved)
    def _():
        swap.start()

    @pl.when(jnp.logical_not(moved))
    def _():
        mine[...] = weight_ref[...]

    step = 256

    def widen(i, carry):
        at = pl.ds(pl.multiple_of(i * step, step), step)
        wide[at, :] = table_ref[at, :].astype(F32)
        return carry

    lax.fori_loop(0, vocab // step, widen, 0)
    ids_copy.wait()

    rows = CHUNKS * chunk
    parts_in_tile = LANES // rows if rows < LANES else 1
    lane0 = lax.rem(m, parts_in_tile) * rows
    span = hots * LANES

    def lookups(ch, g):
        near = ids_ref.at[pl.ds(g * span + lane0 + ch * chunk, (hots - 1) * LANES + chunk)]
        for j in range(chunk):
            total = wide[pl.ds(near[j], 1), :]
            for h in range(1, hots):
                total = total + wide[pl.ds(near[h * LANES + j], 1), :]
            acc[j : j + 1, :] = total

    def dp_copy(ch, k):
        return remote(
            pooled.at[ch, lax.rem(d + k, groups)], recv[ch].at[d], send_sem.at[ch], recv_sem.at[ch], dp_at(k)
        )

    def every(ch):
        some = pl.ds(0, groups - 1)
        return remote(pooled.at[ch, some], recv[ch].at[some], send_sem.at[ch], recv_sem.at[ch], dp_at(1))

    def pool(ch):
        lookups(ch, lax.rem(d + 1, groups))

        def block(k, carry):
            pooled[ch, lax.rem(d + k - 1, groups)] = acc[...].astype(BF16)
            lookups(ch, lax.rem(d + k, groups))
            dp_copy(ch, k - 1).start()
            return carry

        lax.fori_loop(2, groups, block, 0)
        pooled[ch, lax.rem(d + groups - 1, groups)] = acc[...].astype(BF16)
        lookups(ch, d)
        dp_copy(ch, groups - 1).start()
        recv[ch][d] = acc[...].astype(BF16)

    def mp_copy(ch, k):
        to = lax.rem(m + k, members)
        at = pl.ds(ch * chunk, chunk)
        return remote(packed.at[ch, to], emb_ref.at[m, at], mp_send.at[ch, k - 1], mp_recv.at[ch, k - 1], mp_at(k))

    def spread(ch):
        every(ch).wait_recv()
        for p in range(groups):
            packed[ch, p // per, :, (p % per) * width : (p % per + 1) * width] = recv[ch][order_ref[p]]
        emb_ref[m, ch * chunk : (ch + 1) * chunk, :] = packed[ch, m]
        for k in range(1, members):
            mp_copy(ch, k).start()

    def at_xyz(y, x, z):
        return (index_of(sizes, y, x, z, c), m)

    right, left = lax.rem(x + 1, nx), lax.rem(x + nx - 1, nx)
    upper, lower = lax.rem(y + 1, ny), lax.rem(y + ny - 1, ny)
    half = mine.shape[1] // 2
    first, second = pl.ds(0, half), pl.ds(half, half)

    def below():
        other = 1 - z
        return [
            remote(mine.at[0], quarter_ref.at[0, x, z], w_send.at[1], w_recv.at[1], at_xyz(y, x, other)),
            remote(mine.at[1], quarter_ref.at[1, y, z], w_send.at[2], w_recv.at[2], at_xyz(y, x, other)),
        ]

    def beside():
        copies = []
        if nx > 1:
            own = quarter_ref.at[0, x]
            copies.append(remote(own, own, w_send.at[3], w_recv.at[3], at_xyz(y, right, z)))
            copies.append(remote(own, own, w_send.at[4], w_recv.at[4], at_xyz(y, left, z)))
        own = quarter_ref.at[1, y]
        copies.append(remote(own, own, w_send.at[5], w_recv.at[5], at_xyz(upper, x, z)))
        copies.append(remote(own, own, w_send.at[6], w_recv.at[6], at_xyz(lower, x, z)))
        return copies

    def relayed():
        copies = []
        if nx > 1:
            part = quarter_ref.at[0, left, :, first]
            copies.append(remote(part, part, w_send.at[7], w_recv.at[7], at_xyz(y, right, z)))
            part = quarter_ref.at[0, right, :, second]
            copies.append(remote(part, part, w_send.at[8], w_recv.at[8], at_xyz(y, left, z)))
        part = quarter_ref.at[1, lower, :, first]
        copies.append(remote(part, part, w_send.at[9], w_recv.at[9], at_xyz(upper, x, z)))
        part = quarter_ref.at[1, upper, :, second]
        copies.append(remote(part, part, w_send.at[10], w_recv.at[10], at_xyz(lower, x, z)))
        return copies

    def start(copies):
        for copy in copies:
            copy.start()

    def wait(copies):
        for copy in copies:
            copy.wait()

    pool(0)

    @pl.when(moved)
    def _():
        swap.wait()

    if nz > 1:
        start(below())
    quarter_ref[0, x, z] = mine[0]
    quarter_ref[1, y, z] = mine[1]
    pool(1)
    spread(0)
    if nz > 1:
        wait(below())
    start(beside())
    pool(2)
    spread(1)
    wait(beside())
    start(relayed())
    pool(3)
    spread(2)
    spread(3)
    wait(relayed())
    for ch in range(CHUNKS):
        every(ch).wait_send()
        for k in range(1, members):
            mp_copy(ch, k).wait()


def regrouped(ids, order, table, weight, groups, members, hots, rows):
    vocab, width = table.shape
    per = groups // members
    chunk = rows // CHUNKS
    ny, nx, nz, _ = torus(groups, members)
    depth, units = weight.shape[1:]
    return pl.pallas_call(
        functools.partial(regroup_kernel, groups, members, hots),
        out_shape=[
            jax.ShapeDtypeStruct((members, rows, per * width), BF16),
            jax.ShapeDtypeStruct((2, max(ny, nx), nz, depth, units), BF16),
        ],
        in_specs=[ANY, SCALARS, WHOLE, WHOLE],
        out_specs=[WHOLE, WHOLE],
        scratch_shapes=[
            pltpu.SMEM(ids.shape, jnp.int32),
            VMEM((vocab, width), F32),
            VMEM((chunk, width), F32),
            VMEM((CHUNKS, groups, chunk, width), BF16),
            [VMEM((groups, chunk, width), BF16) for _ in range(CHUNKS)],
            VMEM((CHUNKS, members, chunk, per * width), BF16),
            VMEM((2, depth, units), BF16),
            DMA,
            DMA((CHUNKS,)),
            DMA((CHUNKS,)),
            DMA((CHUNKS, members - 1)),
            DMA((CHUNKS, members - 1)),
            DMA((11,)),
            DMA((11,)),
        ],
        compiler_params=pltpu.CompilerParams(collective_id=0, has_side_effects=True),
        name="regroup",
    )(ids, order, table, weight)


def cross_kernel(
    groups, members, emb_ref, quarter_ref, down_hbm, up_hbm, bias_ref, tower_bias_ref, out_ref,
    down_ref, up_ref, tower_ref, part, arrived, proj, crossed, sums, partial_units, units_in,
    load_sem, send_sem, recv_sem, w_send, w_recv,
):
    d = lax.axis_index("dp")
    m = lax.axis_index("mp")
    rows, cols = emb_ref.shape
    layers, _, rank = down_ref.shape
    height = rows // GROUPS
    share = height // members
    units = out_ref.shape[1]
    sizes = torus(groups, members)
    ny, nx, nz, nc = sizes
    y, x, z, c = place(sizes, d)

    loads = []
    for layer in range(layers):
        loads.append(pltpu.make_async_copy(down_hbm.at[layer], down_ref.at[layer], load_sem.at[2 * layer]))
        loads.append(pltpu.make_async_copy(up_hbm.at[layer], up_ref.at[layer], load_sem.at[2 * layer + 1]))
    loads.append(pltpu.make_async_copy(
        quarter_ref.at[0, pl.ds(0, nx)], tower_ref.at[y, :, :, c, 0], load_sem.at[2 * layers]
    ))
    loads.append(pltpu.make_async_copy(
        quarter_ref.at[1, pl.ds(0, ny)], tower_ref.at[:, x, :, c, 1], load_sem.at[2 * layers + 1]
    ))
    for load in loads:
        load.start()

    def mp_at(k):
        return (d, lax.rem(m + k, members))

    def at_xyc(y, x, c):
        return (index_of(sizes, y, x, z, c), m)

    right, left = lax.rem(x + 1, nx), lax.rem(x + nx - 1, nx)
    upper, lower = lax.rem(y + 1, ny), lax.rem(y + ny - 1, ny)
    near = [mp_at(k) for k in range(1, members)]
    near += [at_xyc(upper, x, c), at_xyc(lower, x, c)]
    if nx > 1:
        near += [at_xyc(y, right, c), at_xyc(y, left, c)]
    if nc > 1:
        near.append(at_xyc(y, x, 1 - c))
    for device in near:
        signal(device)
    pl.semaphore_wait(pltpu.get_barrier_semaphore(), len(near))

    def first_way():
        to = tower_ref.at[y, :, :, c, 0]
        src = quarter_ref.at[0, pl.ds(0, nx)]
        copies = [
            remote(src, to, w_send.at[0], w_recv.at[0], at_xyc(upper, x, c)),
            remote(src, to, w_send.at[1], w_recv.at[1], at_xyc(lower, x, c)),
        ]
        if nx > 1:
            to = tower_ref.at[:, x, :, c, 1]
            src = quarter_ref.at[1, pl.ds(0, ny)]
            copies.append(remote(src, to, w_send.at[2], w_recv.at[2], at_xyc(y, right, c)))
            copies.append(remote(src, to, w_send.at[3], w_recv.at[3], at_xyc(y, left, c)))
        return copies

    depth = quarter_ref.shape[3]
    first, second = pl.ds(0, depth // 2), pl.ds(depth // 2, depth // 2)

    def second_way():
        part = tower_ref.at[lower, :, :, c, 0, first]
        copies = [remote(part, part, w_send.at[4], w_recv.at[4], at_xyc(upper, x, c))]
        part = tower_ref.at[upper, :, :, c, 0, second]
        copies.append(remote(part, part, w_send.at[5], w_recv.at[5], at_xyc(lower, x, c)))
        if nx > 1:
            part = tower_ref.at[:, left, :, c, 1, first]
            copies.append(remote(part, part, w_send.at[6], w_recv.at[6], at_xyc(y, right, c)))
            part = tower_ref.at[:, right, :, c, 1, second]
            copies.append(remote(part, part, w_send.at[7], w_recv.at[7], at_xyc(y, left, c)))
        return copies

    def pair():
        if nc == 1:
            return []
        part = tower_ref.at[:, :, :, c]
        return [remote(part, part, w_send.at[8], w_recv.at[8], at_xyc(y, x, 1 - c))]

    def start(copies):
        for copy in copies:
            copy.start()

    def wait(copies):
        for copy in copies:
            copy.wait()

    def rows_of(g):
        return pl.ds(g * height, height)

    def scatter(layer, g):
        i = layer * GROUPS + g
        return [
            remote(
                part.at[i, lax.rem(m + k, members)],
                arrived.at[i, k - 1],
                send_sem.at[2 * i, k - 1],
                recv_sem.at[2 * i, k - 1],
                mp_at(k),
            )
            for k in range(1, members)
        ]

    def gather(layer, g):
        i = layer * GROUPS + g
        return [
            remote(
                proj.at[i, m], proj.at[i, m], send_sem.at[2 * i + 1, k - 1], recv_sem.at[2 * i + 1, k - 1], mp_at(k)
            )
            for k in range(1, members)
        ]

    def project(layer, g):
        source = emb_ref if layer == 0 else crossed
        product = jnp.dot(source[rows_of(g), :], down_ref[layer], preferred_element_type=F32)
        i = layer * GROUPS + g
        part[i] = product.astype(BF16).reshape(members, share, rank)
        start(scatter(layer, g))

    def add_up(layer, g):
        i = layer * GROUPS + g
        wait(scatter(layer, g))
        total = part[i, m].astype(F32)
        for k in range(1, members):
            total = total + arrived[i, k - 1].astype(F32)
        proj[i, m] = total.astype(BF16)
        start(gather(layer, g))

    tile = min(512, cols)

    def lift(layer, g):
        i = layer * GROUPS + g
        wait(gather(layer, g))
        source = emb_ref if layer == 0 else crossed
        projected = proj[i].reshape(height, rank)
        here = rows_of(g)

        def columns(j, carry):
            at = pl.ds(pl.multiple_of(j * tile, tile), tile)
            lifted = lax.dot_general(
                projected, up_ref[layer, at, :], (((1,), (1,)), ((), ())), preferred_element_type=F32
            )
            value = emb_ref[here, at].astype(F32) * (lifted + bias_ref[layer : layer + 1, at])
            crossed[here, at] = (value + source[here, at].astype(F32)).astype(BF16)
            return carry

        lax.fori_loop(0, cols // tile, columns, 0)

    def tower(g, block):
        weights = tower_ref[block].reshape(cols, units)
        return jnp.dot(crossed[rows_of(g), :], weights, preferred_element_type=F32)

    def exchange(g, k):
        i = 2 * layers * GROUPS + g
        return remote(
            partial_units.at[g, k - 1], units_in.at[g, k - 1], send_sem.at[i, k - 1], recv_sem.at[i, k - 1], mp_at(k)
        )

    start(first_way())
    loads[0].wait()
    for g in range(GROUPS):
        project(0, g)
    for g in range(GROUPS):
        add_up(0, g)
    wait(first_way())
    start(second_way())
    loads[1].wait()
    loads[2].wait()
    for layer in range(1, layers):
        for g in range(GROUPS):
            lift(layer - 1, g)
            project(layer, g)
        if layer == 1:
            wait(second_way())
            for load in loads[2 * layers :]:
                load.wait()
            start(pair())
        for g in range(GROUPS):
            add_up(layer, g)
    for load in loads[3 : 2 * layers]:
        load.wait()
    for g in range(GROUPS):
        lift(layers - 1, g)
        if g == 0:
            wait(pair())

        def send_units(k, carry, g=g):
            partial_units[g, k - 1] = tower(g, lax.rem(m + k, members)).astype(BF16)
            exchange(g, k).start()
            return carry

        lax.fori_loop(1, members, send_units, 0)
        sums[rows_of(g), :] = tower(g, m) + tower_bias_ref[...]
    for g in range(GROUPS):
        total = sums[rows_of(g), :]
        for k in range(1, members):
            exchange(g, k).wait()
            total = total + units_in[g, k - 1].astype(F32)
        out_ref[rows_of(g), :] = jnp.maximum(total, 0.0).astype(BF16)


def crossed_and_towered(emb, quarter, down, up, bias, tower_bias, groups, members):
    rows, cols = emb.shape
    layers, _, rank = down.shape
    depth, units = quarter.shape[3:]
    height = rows // GROUPS
    share = height // members
    steps = layers * GROUPS
    phases = 2 * steps + GROUPS
    ny, nx, nz, nc = torus(groups, members)
    return pl.pallas_call(
        functools.partial(cross_kernel, groups, members),
        out_shape=jax.ShapeDtypeStruct((rows, units), BF16),
        in_specs=[WHOLE, ANY, ANY, ANY, WHOLE, WHOLE],
        out_specs=WHOLE,
        scratch_shapes=[
            VMEM(down.shape, BF16),
            VMEM(up.shape, BF16),
            VMEM((ny, nx, nz, nc, 2, depth, units), BF16),
            VMEM((steps, members, share, rank), BF16),
            VMEM((steps, members - 1, share, rank), BF16),
            VMEM((steps, members, share, rank), BF16),
            VMEM((rows, cols), BF16),
            VMEM((rows, units), F32),
            VMEM((GROUPS, members - 1, height, units), BF16),
            VMEM((GROUPS, members - 1, height, units), BF16),
            DMA((2 * layers + 2,)),
            DMA((phases, members - 1)),
            DMA((phases, members - 1)),
            DMA((9,)),
            DMA((9,)),
        ],
        compiler_params=pltpu.CompilerParams(
            collective_id=1, has_side_effects=True, vmem_limit_bytes=48 * 1024 * 1024
        ),
        name="cross",
    )(emb, quarter, down, up, bias, tower_bias)


def body(groups, members, feature_ids, tables, table_of_feature, cross_down, cross_up, cross_bias, tower_weight, tower_bias):
    m = lax.axis_index("mp")
    _, batch, hots = feature_ids.shape
    rows = batch // (groups * members)
    parts = max(1, LANES // rows)
    tiles = jnp.transpose(jnp.transpose(feature_ids[0]).reshape(hots, batch // LANES, LANES), (1, 0, 2))
    tiles = tiles.reshape(groups, members // parts, hots, LANES)
    own_ids = lax.dynamic_index_in_dim(tiles, m // parts, 1, keepdims=False).reshape(-1)
    depth, units = tower_weight.shape
    weight = tower_weight.reshape(2, depth // 2, units)
    emb, quarter = regrouped(own_ids, table_of_feature, tables[0], weight, groups, members, hots, rows)
    emb = emb.reshape(members * rows, -1)
    return crossed_and_towered(
        emb, quarter, cross_down, cross_up, cross_bias, tower_bias.reshape(1, -1), groups, members
    )


def solution(mesh):
    groups, members = mesh.shape["dp"], mesh.shape["mp"]
    return jax.shard_map(
        functools.partial(body, groups, members),
        mesh=mesh,
        in_specs=(
            P("dp", None, None),
            P("dp", None, None),
            P(),
            P(None, "mp", None),
            P(None, "mp", None),
            P(None, "mp"),
            P("dp", "mp"),
            P("mp"),
        ),
        out_specs=P("dp", "mp"),
        check_vma=False,
    )
```

```python
import functools

import jax
import jax.numpy as jnp
from jax import lax
from jax.experimental import pallas as pl
from jax.experimental.pallas import tpu as pltpu
from jax.sharding import PartitionSpec as P

MESH = pl.DeviceIdType.MESH
VMEM = pltpu.VMEM
DMA = pltpu.SemaphoreType.DMA
F32 = jnp.float32
BF16 = jnp.bfloat16
WHOLE = pl.BlockSpec(memory_space=pltpu.VMEM)
SCALARS = pl.BlockSpec(memory_space=pltpu.SMEM)
ANY = pl.BlockSpec(memory_space=pl.ANY)
LANES = 128
CHUNKS = 4
GROUPS = 2


def torus(groups, members):
    rest = groups // members
    across = min(4, rest)
    rest //= across
    below = min(2, rest)
    return members, across, below, rest // below


def place(sizes, d):
    _, nx, nz, nc = sizes
    return d // (nx * nz * nc), lax.rem(d // (nz * nc), nx), lax.rem(d // nc, nz), lax.rem(d, nc)


def index_of(sizes, y, x, z, c):
    _, nx, nz, nc = sizes
    return ((y * nx + x) * nz + z) * nc + c


def signal(device):
    pl.semaphore_signal(pltpu.get_barrier_semaphore(), inc=1, device_id=device, device_id_type=MESH)


def remote(src, dst, send, recv, device):
    return pltpu.make_async_remote_copy(
        src_ref=src, dst_ref=dst, send_sem=send, recv_sem=recv, device_id=device, device_id_type=MESH
    )


def kernel(
    groups, members, hots, ids_hbm, order_ref, table_hbm, weight_hbm, down_hbm, up_hbm, bias_hbm, tower_bias_hbm,
    out_ref, ids_ref, table_ref, wide, acc, pooled, recv, packed, emb_ref, mine, quarter_ref, tower_ref,
    down_ref, up_ref, bias_ref, tower_bias_ref, part, arrived, proj, crossed, sums, partial_units, units_in,
    load_sem, dp_send, dp_recv, mp_send, mp_recv, send_sem, recv_sem, w_send, w_recv,
):
    d = lax.axis_index("dp")
    m = lax.axis_index("mp")
    vocab, width = table_ref.shape
    chunk = pooled.shape[2]
    per = groups // members
    rows, cols = emb_ref.shape
    layers, _, rank = down_ref.shape
    height = rows // GROUPS
    share = height // members
    units = out_ref.shape[1]
    sizes = torus(groups, members)
    ny, nx, nz, nc = sizes
    y, x, z, c = place(sizes, d)

    def start(copies):
        for copy in copies:
            copy.start()

    def wait(copies):
        for copy in copies:
            copy.wait()

    pairs = [(ids_hbm, ids_ref), (table_hbm, table_ref), (bias_hbm, bias_ref), (tower_bias_hbm, tower_bias_ref)]
    for layer in range(layers):
        pairs.append((down_hbm.at[layer], down_ref.at[layer]))
        pairs.append((up_hbm.at[layer], up_ref.at[layer]))
    loads = [pltpu.make_async_copy(a, b, load_sem.at[i]) for i, (a, b) in enumerate(pairs)]
    own_weight = pltpu.make_async_copy(weight_hbm, mine, load_sem.at[len(pairs)])
    start(loads[:2])

    def dp_at(k):
        return (lax.rem(d + k, groups), m)

    def mp_at(k):
        return (d, lax.rem(m + k, members))

    turned = (m * per + lax.rem(d, per), d // per)
    moved = d // per != m
    for count, device in ((groups, dp_at), (members, mp_at)):

        def greet(k, carry, device=device):
            signal(device(k))
            return carry

        lax.fori_loop(1, count, greet, 0)

    @pl.when(moved)
    def _():
        signal(turned)

    loads[1].wait()
    step = 256

    def widen(i, carry):
        at = pl.ds(pl.multiple_of(i * step, step), step)
        wide[at, :] = table_ref[at, :].astype(F32)
        return carry

    lax.fori_loop(0, vocab // step, widen, 0)
    loads[0].wait()

    local = CHUNKS * chunk
    parts_in_tile = LANES // local if local < LANES else 1
    lane0 = lax.rem(m, parts_in_tile) * local
    span = hots * LANES

    def lookups(ch, g):
        base = g * span + lane0

        def row(h, j):
            skipped = h * LANES + ch * chunk + j
            return wide[pl.ds(ids_ref.at[pl.ds(skipped, ids_ref.shape[0] - skipped)][base], 1), :]

        for j in range(chunk):
            total = row(0, j)
            for h in range(1, hots):
                total = total + row(h, j)
            acc[j : j + 1, :] = total

    def dp_copy(ch, k):
        return remote(
            pooled.at[ch, lax.rem(d + k, groups)], recv[ch].at[d], dp_send.at[ch], dp_recv.at[ch], dp_at(k)
        )

    def every(ch):
        some = pl.ds(0, groups - 1)
        return remote(pooled.at[ch, some], recv[ch].at[some], dp_send.at[ch], dp_recv.at[ch], dp_at(1))

    def blocks(ch, low, high, send=True):
        def block(k, carry):
            pooled[ch, lax.rem(d + k - 1, groups)] = acc[...].astype(BF16)
            lookups(ch, lax.rem(d + k, groups))
            if send:
                dp_copy(ch, k - 1).start()
            return carry

        lax.fori_loop(low, high, block, 0)

    def last_block(ch):
        pooled[ch, lax.rem(d + groups - 1, groups)] = acc[...].astype(BF16)
        lookups(ch, d)
        dp_copy(ch, groups - 1).start()
        recv[ch][d] = acc[...].astype(BF16)

    def emb_rows(ch, member):
        return pl.ds(pl.multiple_of((ch * members + member) * chunk, chunk), chunk)

    def mp_copy(ch, k):
        to = lax.rem(m + k, members)
        return remote(
            packed.at[ch, to], emb_ref.at[emb_rows(ch, m)], mp_send.at[ch, k - 1], mp_recv.at[ch, k - 1], mp_at(k)
        )

    def spread(ch):
        every(ch).wait_recv()
        for p in range(groups):
            packed[ch, p // per, :, (p % per) * width : (p % per + 1) * width] = recv[ch][order_ref[p]]
        for k in range(1, members):
            mp_copy(ch, k).start()
        emb_ref[emb_rows(ch, m), :] = packed[ch, m]

    swap = remote(weight_hbm, mine, w_send.at[0], w_recv.at[0], turned)
    right, left = lax.rem(x + 1, nx), lax.rem(x + nx - 1, nx)
    upper, lower = lax.rem(y + 1, ny), lax.rem(y + ny - 1, ny)
    depth = mine.shape[1]
    first, second = pl.ds(0, depth // 2), pl.ds(depth // 2, depth // 2)

    def at(y, x, z, c):
        return (index_of(sizes, y, x, z, c), m)

    to_right, to_left = at(y, right, z, c), at(y, left, z, c)
    to_upper, to_lower = at(upper, x, z, c), at(lower, x, z, c)

    def send_all(number, moves):
        return [
            remote(src, dst, w_send.at[number + i], w_recv.at[number + i], device)
            for i, (src, dst, device) in enumerate(moves)
        ]

    def below():
        if nz == 1:
            return []
        to = at(y, x, 1 - z, c)
        return send_all(1, [(mine.at[0], quarter_ref.at[0, x, z], to), (mine.at[1], quarter_ref.at[1, y, z], to)])

    def beside():
        own = quarter_ref.at[1, y]
        moves = [(own, own, to_upper), (own, own, to_lower)]
        if nx > 1:
            own = quarter_ref.at[0, x]
            moves += [(own, own, to_right), (own, own, to_left)]
        return send_all(3, moves)

    def relayed():
        a, b = quarter_ref.at[1, lower, :, first], quarter_ref.at[1, upper, :, second]
        moves = [(a, a, to_upper), (b, b, to_lower)]
        if nx > 1:
            a, b = quarter_ref.at[0, left, :, first], quarter_ref.at[0, right, :, second]
            moves += [(a, a, to_right), (b, b, to_left)]
        return send_all(7, moves)

    def first_way():
        src, to = quarter_ref.at[0, pl.ds(0, nx)], tower_ref.at[y, :, :, c, 0]
        moves = [(src, to, to_upper), (src, to, to_lower)]
        if nx > 1:
            src, to = quarter_ref.at[1, pl.ds(0, ny)], tower_ref.at[:, x, :, c, 1]
            moves += [(src, to, to_right), (src, to, to_left)]
        return send_all(11, moves)

    def second_way():
        a, b = tower_ref.at[lower, :, :, c, 0, first], tower_ref.at[upper, :, :, c, 0, second]
        moves = [(a, a, to_upper), (b, b, to_lower)]
        if nx > 1:
            a, b = tower_ref.at[:, left, :, c, 1, first], tower_ref.at[:, right, :, c, 1, second]
            moves += [(a, a, to_right), (b, b, to_left)]
        return send_all(15, moves)

    def pair():
        if nc == 1:
            return []
        both = tower_ref.at[:, :, :, c]
        return send_all(19, [(both, both, at(y, x, z, 1 - c))])

    def rows_of(g):
        return pl.ds(g * height, height)

    def scatter(layer, g):
        i = layer * GROUPS + g
        return [
            remote(
                part.at[i, lax.rem(m + k, members)],
                arrived.at[i, k - 1],
                send_sem.at[2 * i, k - 1],
                recv_sem.at[2 * i, k - 1],
                mp_at(k),
            )
            for k in range(1, members)
        ]

    def gather(layer, g):
        i = layer * GROUPS + g
        return [
            remote(
                proj.at[i, m], proj.at[i, m], send_sem.at[2 * i + 1, k - 1], recv_sem.at[2 * i + 1, k - 1], mp_at(k)
            )
            for k in range(1, members)
        ]

    def project(layer, g):
        source = emb_ref if layer == 0 else crossed
        product = jnp.dot(source[rows_of(g), :], down_ref[layer], preferred_element_type=F32)
        i = layer * GROUPS + g
        part[i] = product.astype(BF16).reshape(members, share, rank)
        start(scatter(layer, g))

    def add_up(layer, g):
        i = layer * GROUPS + g
        wait(scatter(layer, g))
        total = part[i, m].astype(F32)
        for k in range(1, members):
            total = total + arrived[i, k - 1].astype(F32)
        proj[i, m] = total.astype(BF16)
        start(gather(layer, g))

    tile = min(512, cols)

    def lift(layer, g):
        i = layer * GROUPS + g
        wait(gather(layer, g))
        source = emb_ref if layer == 0 else crossed
        projected = proj[i].reshape(height, rank)
        here = rows_of(g)

        def columns(j, carry):
            at = pl.ds(pl.multiple_of(j * tile, tile), tile)
            lifted = lax.dot_general(
                projected, up_ref[layer, at, :], (((1,), (1,)), ((), ())), preferred_element_type=F32
            )
            value = emb_ref[here, at].astype(F32) * (lifted + bias_ref[layer : layer + 1, at])
            crossed[here, at] = (value + source[here, at].astype(F32)).astype(BF16)
            return carry

        lax.fori_loop(0, cols // tile, columns, 0)

    def tower(g, block):
        weights = tower_ref[block].reshape(cols, units)
        return jnp.dot(crossed[rows_of(g), :], weights, preferred_element_type=F32)

    def exchange(g, k):
        i = 2 * layers * GROUPS + g
        return remote(
            partial_units.at[g, k - 1], units_in.at[g, k - 1], send_sem.at[i, k - 1], recv_sem.at[i, k - 1], mp_at(k)
        )

    in_group = CHUNKS // GROUPS

    def project_first(g):
        for ch in range(g * in_group, (g + 1) * in_group):
            for k in range(1, members):
                mp_copy(ch, k).wait_recv()
        project(0, g)

    cuts = [2, 2 + groups // 4, 1 + groups // 2, 1 + 3 * groups // 4, groups]

    lookups(0, lax.rem(d + 1, groups))
    blocks(0, cuts[0], cuts[2], send=False)
    pl.semaphore_wait(
        pltpu.get_barrier_semaphore(), groups + members - 2 + jnp.where(moved, 1, 0).astype(jnp.int32)
    )

    def send_first(k, carry):
        dp_copy(0, k).start()
        return carry

    lax.fori_loop(1, cuts[2] - 1, send_first, 0)

    @pl.when(moved)
    def _():
        swap.start()

    @pl.when(jnp.logical_not(moved))
    def _():
        own_weight.start()

    blocks(0, cuts[2], cuts[4])
    last_block(0)
    start(loads[2:])

    @pl.when(moved)
    def _():
        swap.wait()

    @pl.when(jnp.logical_not(moved))
    def _():
        own_weight.wait()

    start(below())
    quarter_ref[0, x, z] = mine[0]
    quarter_ref[1, y, z] = mine[1]
    for ch in range(1, CHUNKS):
        lookups(ch, lax.rem(d + 1, groups))
        blocks(ch, cuts[0], cuts[3])
        spread(ch - 1)
        if ch == 1:
            wait(below())
            start(beside())
        if ch == 2:
            wait(beside())
            start(relayed())
        if ch == 3:
            wait(relayed())
            start(first_way())
        blocks(ch, cuts[3], cuts[4])
        last_block(ch)
    for load in loads[2:]:
        load.wait()
    project_first(0)
    spread(CHUNKS - 1)
    tower_ref[y, :, :, c, 0] = quarter_ref[0, :nx]
    tower_ref[:, x, :, c, 1] = quarter_ref[1, :ny]
    add_up(0, 0)
    for g in range(1, GROUPS):
        project_first(g)
        add_up(0, g)
    wait(first_way())
    start(second_way())
    for layer in range(1, layers):
        for g in range(GROUPS):
            lift(layer - 1, g)
            project(layer, g)
        if layer == 1:
            wait(second_way())
            start(pair())
        for g in range(GROUPS):
            add_up(layer, g)
    for g in range(GROUPS):
        lift(layers - 1, g)
        if g == 0:
            wait(pair())

        def send_units(k, carry, g=g):
            partial_units[g, k - 1] = tower(g, lax.rem(m + k, members)).astype(BF16)
            exchange(g, k).start()
            return carry

        lax.fori_loop(1, members, send_units, 0)
        sums[rows_of(g), :] = tower(g, m) + tower_bias_ref[...]
    for g in range(GROUPS):
        total = sums[rows_of(g), :]
        for k in range(1, members):
            exchange(g, k).wait()
            total = total + units_in[g, k - 1].astype(F32)
        total = jnp.maximum(total, 0.0).astype(BF16)
        for ch in range(in_group):
            for member in range(members):
                to = (member * CHUNKS + g * in_group + ch) * chunk
                at0 = (ch * members + member) * chunk
                out_ref[to : to + chunk, :] = total[at0 : at0 + chunk, :]
    for ch in range(CHUNKS):
        every(ch).wait_send()
        for k in range(1, members):
            mp_copy(ch, k).wait_send()


def whole(ids, order, table, weight, down, up, bias, tower_bias, groups, members, hots, local):
    vocab, width = table.shape
    per = groups // members
    chunk = local // CHUNKS
    rows, cols = members * local, per * width
    layers, _, rank = down.shape
    depth, units = weight.shape[1:]
    height = rows // GROUPS
    share = height // members
    steps = layers * GROUPS
    phases = 2 * steps + GROUPS
    ny, nx, nz, nc = torus(groups, members)
    return pl.pallas_call(
        functools.partial(kernel, groups, members, hots),
        out_shape=jax.ShapeDtypeStruct((rows, units), BF16),
        in_specs=[ANY, SCALARS] + [ANY] * 6,
        out_specs=WHOLE,
        scratch_shapes=[
            pltpu.SMEM(ids.shape, jnp.int32),
            VMEM((vocab, width), BF16),
            VMEM((vocab, width), F32),
            VMEM((chunk, width), F32),
            VMEM((CHUNKS, groups, chunk, width), BF16),
            [VMEM((groups, chunk, width), BF16) for _ in range(CHUNKS)],
            VMEM((CHUNKS, members, chunk, cols), BF16),
            VMEM((rows, cols), BF16),
            VMEM((2, depth, units), BF16),
            VMEM((2, max(ny, nx), nz, depth, units), BF16),
            VMEM((ny, nx, nz, nc, 2, depth, units), BF16),
            VMEM(down.shape, BF16),
            VMEM(up.shape, BF16),
            VMEM(bias.shape, F32),
            VMEM(tower_bias.shape, F32),
            VMEM((steps, members, share, rank), BF16),
            VMEM((steps, members - 1, share, rank), BF16),
            VMEM((steps, members, share, rank), BF16),
            VMEM((rows, cols), BF16),
            VMEM((rows, units), F32),
            VMEM((GROUPS, members - 1, height, units), BF16),
            VMEM((GROUPS, members - 1, height, units), BF16),
            DMA((2 * layers + 5,)),
            DMA((CHUNKS,)),
            DMA((CHUNKS,)),
            DMA((CHUNKS, members - 1)),
            DMA((CHUNKS, members - 1)),
            DMA((phases, members - 1)),
            DMA((phases, members - 1)),
            DMA((20,)),
            DMA((20,)),
        ],
        compiler_params=pltpu.CompilerParams(
            collective_id=0, has_side_effects=True, vmem_limit_bytes=56 * 1024 * 1024
        ),
        name="whole",
    )(ids, order, table, weight, down, up, bias, tower_bias)


def body(groups, members, feature_ids, tables, table_of_feature, cross_down, cross_up, cross_bias, tower_weight, tower_bias):
    m = lax.axis_index("mp")
    _, batch, hots = feature_ids.shape
    rows = batch // (groups * members)
    parts = max(1, LANES // rows)
    tiles = jnp.transpose(jnp.transpose(feature_ids[0]).reshape(hots, batch // LANES, LANES), (1, 0, 2))
    tiles = tiles.reshape(groups, members // parts, hots, LANES)
    own_ids = lax.dynamic_index_in_dim(tiles, m // parts, 1, keepdims=False).reshape(-1)
    depth, units = tower_weight.shape
    weight = tower_weight.reshape(2, depth // 2, units)
    return whole(
        own_ids, table_of_feature, tables[0], weight, cross_down, cross_up, cross_bias,
        tower_bias.reshape(1, -1), groups, members, hots, rows,
    )


def solution(mesh):
    groups, members = mesh.shape["dp"], mesh.shape["mp"]
    return jax.shard_map(
        functools.partial(body, groups, members),
        mesh=mesh,
        in_specs=(
            P("dp", None, None),
            P("dp", None, None),
            P(),
            P(None, "mp", None),
            P(None, "mp", None),
            P(None, "mp"),
            P("dp", "mp"),
            P("mp"),
        ),
        out_specs=P("dp", "mp"),
        check_vma=False,
    )
```

```python
import functools

import jax
import jax.numpy as jnp
from jax import lax
from jax.experimental import pallas as pl
from jax.experimental.pallas import tpu as pltpu
from jax.sharding import PartitionSpec as P

MESH = pl.DeviceIdType.MESH
VMEM = pltpu.VMEM
DMA = pltpu.SemaphoreType.DMA
F32 = jnp.float32
BF16 = jnp.bfloat16
WHOLE = pl.BlockSpec(memory_space=pltpu.VMEM)
SCALARS = pl.BlockSpec(memory_space=pltpu.SMEM)
ANY = pl.BlockSpec(memory_space=pl.ANY)
LANES = 128
CHUNKS = 4
GROUPS = 2


def torus(groups, members):
    rest = groups // members
    across = min(4, rest)
    rest //= across
    below = min(2, rest)
    return members, across, below, rest // below


def place(sizes, d):
    _, nx, nz, nc = sizes
    return d // (nx * nz * nc), lax.rem(d // (nz * nc), nx), lax.rem(d // nc, nz), lax.rem(d, nc)


def index_of(sizes, y, x, z, c):
    _, nx, nz, nc = sizes
    return ((y * nx + x) * nz + z) * nc + c


def signal(device):
    pl.semaphore_signal(pltpu.get_barrier_semaphore(), inc=1, device_id=device, device_id_type=MESH)


def remote(src, dst, send, recv, device):
    return pltpu.make_async_remote_copy(
        src_ref=src, dst_ref=dst, send_sem=send, recv_sem=recv, device_id=device, device_id_type=MESH
    )


def kernel(
    groups, members, hots, ids_hbm, order_ref, table_hbm, weight_hbm, down_hbm, up_hbm, bias_hbm, tower_bias_hbm,
    out_ref, ids_ref, table_ref, wide, acc, pooled, recv, packed, emb_ref, mine, quarter_ref, tower_ref,
    down_ref, up_ref, bias_ref, tower_bias_ref, part, arrived, proj, crossed, sums, near_units, far_units, far_in, partial_units, units_in,
    load_sem, dp_send, dp_recv, mp_send, mp_recv, send_sem, recv_sem, w_send, w_recv,
):
    d = lax.axis_index("dp")
    m = lax.axis_index("mp")
    vocab, width = table_ref.shape
    chunk = pooled.shape[2]
    per = groups // members
    rows, cols = emb_ref.shape
    layers, _, rank = down_ref.shape
    height = rows // GROUPS
    share = height // members
    units = out_ref.shape[1]
    sizes = torus(groups, members)
    ny, nx, nz, nc = sizes
    y, x, z, c = place(sizes, d)

    def start(copies):
        for copy in copies:
            copy.start()

    def wait(copies):
        for copy in copies:
            copy.wait()

    pairs = [(ids_hbm, ids_ref), (table_hbm, table_ref), (bias_hbm, bias_ref), (tower_bias_hbm, tower_bias_ref)]
    for layer in range(layers):
        pairs.append((down_hbm.at[layer], down_ref.at[layer]))
        pairs.append((up_hbm.at[layer], up_ref.at[layer]))
    loads = [pltpu.make_async_copy(a, b, load_sem.at[i]) for i, (a, b) in enumerate(pairs)]
    own_weight = pltpu.make_async_copy(weight_hbm, mine, load_sem.at[len(pairs)])
    start(loads[:2])

    def dp_at(k):
        return (lax.rem(d + k, groups), m)

    def mp_at(k):
        return (d, lax.rem(m + k, members))

    turned = (m * per + lax.rem(d, per), d // per)
    moved = d // per != m
    for count, device in ((groups, dp_at), (members, mp_at)):

        def greet(k, carry, device=device):
            signal(device(k))
            return carry

        lax.fori_loop(1, count, greet, 0)

    @pl.when(moved)
    def _():
        signal(turned)

    loads[1].wait()
    step = 256

    def widen(i, carry):
        at = pl.ds(pl.multiple_of(i * step, step), step)
        wide[at, :] = table_ref[at, :].astype(F32)
        return carry

    lax.fori_loop(0, vocab // step, widen, 0)
    loads[0].wait()

    local = CHUNKS * chunk
    parts_in_tile = LANES // local if local < LANES else 1
    lane0 = lax.rem(m, parts_in_tile) * local
    span = hots * LANES

    def lookups(ch, g):
        base = g * span + lane0

        def row(h, j):
            skipped = h * LANES + ch * chunk + j
            return wide[pl.ds(ids_ref.at[pl.ds(skipped, ids_ref.shape[0] - skipped)][base], 1), :]

        for j in range(chunk):
            total = row(0, j)
            for h in range(1, hots):
                total = total + row(h, j)
            acc[j : j + 1, :] = total

    def dp_copy(ch, k):
        return remote(
            pooled.at[ch, lax.rem(d + k, groups)], recv[ch].at[d], dp_send.at[ch], dp_recv.at[ch], dp_at(k)
        )

    def every(ch):
        some = pl.ds(0, groups - 1)
        return remote(pooled.at[ch, some], recv[ch].at[some], dp_send.at[ch], dp_recv.at[ch], dp_at(1))

    def blocks(ch, low, high, send=True):
        def block(k, carry):
            pooled[ch, lax.rem(d + k - 1, groups)] = acc[...].astype(BF16)
            lookups(ch, lax.rem(d + k, groups))
            if send:
                dp_copy(ch, k - 1).start()
            return carry

        lax.fori_loop(low, high, block, 0)

    def last_block(ch):
        pooled[ch, lax.rem(d + groups - 1, groups)] = acc[...].astype(BF16)
        lookups(ch, d)
        dp_copy(ch, groups - 1).start()
        recv[ch][d] = acc[...].astype(BF16)

    def emb_rows(ch, member):
        return pl.ds(pl.multiple_of((ch * members + member) * chunk, chunk), chunk)

    def mp_copy(ch, k):
        to = lax.rem(m + k, members)
        return remote(
            packed.at[ch, to], emb_ref.at[emb_rows(ch, m)], mp_send.at[ch, k - 1], mp_recv.at[ch, k - 1], mp_at(k)
        )

    def spread(ch):
        every(ch).wait_recv()
        for p in range(groups):
            packed[ch, p // per, :, (p % per) * width : (p % per + 1) * width] = recv[ch][order_ref[p]]
        for k in range(1, members):
            mp_copy(ch, k).start()
        emb_ref[emb_rows(ch, m), :] = packed[ch, m]

    swap = remote(weight_hbm, mine, w_send.at[0], w_recv.at[0], turned)
    right, left = lax.rem(x + 1, nx), lax.rem(x + nx - 1, nx)
    upper, lower = lax.rem(y + 1, ny), lax.rem(y + ny - 1, ny)
    depth = mine.shape[1]
    first, second = pl.ds(0, depth // 2), pl.ds(depth // 2, depth // 2)

    def at(y, x, z, c):
        return (index_of(sizes, y, x, z, c), m)

    to_right, to_left = at(y, right, z, c), at(y, left, z, c)
    to_upper, to_lower = at(upper, x, z, c), at(lower, x, z, c)

    def send_all(number, moves):
        return [
            remote(src, dst, w_send.at[number + i], w_recv.at[number + i], device)
            for i, (src, dst, device) in enumerate(moves)
        ]

    def below():
        if nz == 1:
            return []
        to = at(y, x, 1 - z, c)
        return send_all(1, [(mine.at[0], quarter_ref.at[0, x, z], to), (mine.at[1], quarter_ref.at[1, y, z], to)])

    def beside():
        own = quarter_ref.at[1, y]
        moves = [(own, own, to_upper), (own, own, to_lower)]
        if nx > 1:
            own = quarter_ref.at[0, x]
            moves += [(own, own, to_right), (own, own, to_left)]
        return send_all(3, moves)

    def relayed():
        a, b = quarter_ref.at[1, lower, :, first], quarter_ref.at[1, upper, :, second]
        moves = [(a, a, to_upper), (b, b, to_lower)]
        if nx > 1:
            a, b = quarter_ref.at[0, left, :, first], quarter_ref.at[0, right, :, second]
            moves += [(a, a, to_right), (b, b, to_left)]
        return send_all(7, moves)

    def first_way():
        src, to = quarter_ref.at[0, pl.ds(0, nx)], tower_ref.at[y, :, :, c, 0]
        moves = [(src, to, to_upper), (src, to, to_lower)]
        if nx > 1:
            src, to = quarter_ref.at[1, pl.ds(0, ny)], tower_ref.at[:, x, :, c, 1]
            moves += [(src, to, to_right), (src, to, to_left)]
        return send_all(11, moves)

    def second_way():
        a, b = tower_ref.at[lower, :, :, c, 0, first], tower_ref.at[upper, :, :, c, 0, second]
        moves = [(a, a, to_upper), (b, b, to_lower)]
        if nx > 1:
            a, b = tower_ref.at[:, left, :, c, 1, first], tower_ref.at[:, right, :, c, 1, second]
            moves += [(a, a, to_right), (b, b, to_left)]
        return send_all(15, moves)

    def pair():
        if nc == 1:
            return []
        both = tower_ref.at[:, :, :, c]
        return send_all(19, [(both, both, at(y, x, z, 1 - c))])

    def rows_of(g):
        return pl.ds(g * height, height)

    def scatter(layer, g):
        i = layer * GROUPS + g
        return [
            remote(
                part.at[i, lax.rem(m + k, members)],
                arrived.at[i, k - 1],
                send_sem.at[2 * i, k - 1],
                recv_sem.at[2 * i, k - 1],
                mp_at(k),
            )
            for k in range(1, members)
        ]

    def gather(layer, g):
        i = layer * GROUPS + g
        return [
            remote(
                proj.at[i, m], proj.at[i, m], send_sem.at[2 * i + 1, k - 1], recv_sem.at[2 * i + 1, k - 1], mp_at(k)
            )
            for k in range(1, members)
        ]

    def project(layer, g):
        source = emb_ref if layer == 0 else crossed
        product = jnp.dot(source[rows_of(g), :], down_ref[layer], preferred_element_type=F32)
        i = layer * GROUPS + g
        part[i] = product.astype(BF16).reshape(members, share, rank)
        start(scatter(layer, g))

    def add_up(layer, g):
        i = layer * GROUPS + g
        wait(scatter(layer, g))
        total = part[i, m].astype(F32)
        for k in range(1, members):
            total = total + arrived[i, k - 1].astype(F32)
        proj[i, m] = total.astype(BF16)
        start(gather(layer, g))

    tile = min(512, cols)

    def lift(layer, g):
        i = layer * GROUPS + g
        wait(gather(layer, g))
        source = emb_ref if layer == 0 else crossed
        projected = proj[i].reshape(height, rank)
        here = rows_of(g)

        def columns(j, carry):
            at = pl.ds(pl.multiple_of(j * tile, tile), tile)
            lifted = lax.dot_general(
                projected, up_ref[layer, at, :], (((1,), (1,)), ((), ())), preferred_element_type=F32
            )
            value = emb_ref[here, at].astype(F32) * (lifted + bias_ref[layer : layer + 1, at])
            crossed[here, at] = (value + source[here, at].astype(F32)).astype(BF16)
            return carry

        lax.fori_loop(0, cols // tile, columns, 0)

    def tower(g, block):
        weights = tower_ref[block].reshape(cols, units)
        return jnp.dot(crossed[rows_of(g), :], weights, preferred_element_type=F32)

    tower_phase = 2 * layers * GROUPS
    top, low = pl.ds(0, height // 2), pl.ds(height // 2, height // 2)

    def opposite(g):
        i = tower_phase + 2 * g
        return [
            remote(far_units.at[g, top], far_in.at[g, 0], send_sem.at[i, 0], recv_sem.at[i, 0], mp_at(1)),
            remote(far_units.at[g, low], far_in.at[g, 1], send_sem.at[i, 1], recv_sem.at[i, 1], mp_at(members - 1)),
        ]

    def neighbours(g):
        i = tower_phase + 2 * g + 1
        return [
            remote(partial_units.at[g, 0], units_in.at[g, 0], send_sem.at[i, 0], recv_sem.at[i, 0], mp_at(1)),
            remote(partial_units.at[g, 1], units_in.at[g, 1], send_sem.at[i, 1], recv_sem.at[i, 1], mp_at(members - 1)),
        ]

    def send_far(g):
        far_units[g] = tower(g, lax.rem(m + 2, members)).astype(BF16)
        start(opposite(g))

    def send_near(g):
        for side, k in enumerate((1, members - 1)):
            near_units[side] = tower(g, lax.rem(m + k, members))
        wait(opposite(g))
        partial_units[g, 0, top, :] = (near_units[0, top, :] + far_in[g, 0].astype(F32)).astype(BF16)
        partial_units[g, 0, low, :] = near_units[0, low, :].astype(BF16)
        partial_units[g, 1, top, :] = near_units[1, top, :].astype(BF16)
        partial_units[g, 1, low, :] = (near_units[1, low, :] + far_in[g, 1].astype(F32)).astype(BF16)
        start(neighbours(g))

    in_group = CHUNKS // GROUPS

    def project_first(g):
        for ch in range(g * in_group, (g + 1) * in_group):
            for k in range(1, members):
                mp_copy(ch, k).wait_recv()
        project(0, g)

    cuts = [2, 2 + groups // 4, 1 + groups // 2, 1 + 3 * groups // 4, groups]

    lookups(0, lax.rem(d + 1, groups))
    blocks(0, cuts[0], cuts[2], send=False)
    pl.semaphore_wait(
        pltpu.get_barrier_semaphore(), groups + members - 2 + jnp.where(moved, 1, 0).astype(jnp.int32)
    )

    def send_first(k, carry):
        dp_copy(0, k).start()
        return carry

    lax.fori_loop(1, cuts[2] - 1, send_first, 0)

    @pl.when(moved)
    def _():
        swap.start()

    @pl.when(jnp.logical_not(moved))
    def _():
        own_weight.start()

    blocks(0, cuts[2], cuts[4])
    last_block(0)
    start(loads[2:])

    @pl.when(moved)
    def _():
        swap.wait()

    @pl.when(jnp.logical_not(moved))
    def _():
        own_weight.wait()

    start(below())
    quarter_ref[0, x, z] = mine[0]
    quarter_ref[1, y, z] = mine[1]
    for ch in range(1, CHUNKS):
        lookups(ch, lax.rem(d + 1, groups))
        blocks(ch, cuts[0], cuts[3])
        spread(ch - 1)
        blocks(ch, cuts[3], cuts[4])
        last_block(ch)
        if ch == 1:
            wait(below())
            start(beside())
        if ch == 2:
            wait(beside())
            start(relayed())
    for load in loads[2:]:
        load.wait()
    project_first(0)
    spread(CHUNKS - 1)
    wait(relayed())
    start(first_way())
    tower_ref[y, :, :, c, 0] = quarter_ref[0, :nx]
    tower_ref[:, x, :, c, 1] = quarter_ref[1, :ny]
    add_up(0, 0)
    for g in range(1, GROUPS):
        project_first(g)
        add_up(0, g)
    wait(first_way())
    start(second_way())
    for layer in range(1, layers):
        for g in range(GROUPS):
            lift(layer - 1, g)
            project(layer, g)
        if layer == 1:
            wait(second_way())
            start(pair())
        for g in range(GROUPS):
            add_up(layer, g)
    for g in range(GROUPS):
        lift(layers - 1, g)
        if g == 0:
            wait(pair())
        send_far(g)
    for g in range(GROUPS):
        send_near(g)
    for g in range(GROUPS):
        sums[rows_of(g), :] = tower(g, m) + tower_bias_ref[...]
    for g in range(GROUPS):
        wait(neighbours(g))
        total = sums[rows_of(g), :] + units_in[g, 0].astype(F32) + units_in[g, 1].astype(F32)
        total = jnp.maximum(total, 0.0).astype(BF16)
        for ch in range(in_group):
            for member in range(members):
                to = (member * CHUNKS + g * in_group + ch) * chunk
                at0 = (ch * members + member) * chunk
                out_ref[to : to + chunk, :] = total[at0 : at0 + chunk, :]
    for ch in range(CHUNKS):
        every(ch).wait_send()
        for k in range(1, members):
            mp_copy(ch, k).wait_send()


def whole(ids, order, table, weight, down, up, bias, tower_bias, groups, members, hots, local):
    vocab, width = table.shape
    per = groups // members
    chunk = local // CHUNKS
    rows, cols = members * local, per * width
    layers, _, rank = down.shape
    depth, units = weight.shape[1:]
    height = rows // GROUPS
    share = height // members
    steps = layers * GROUPS
    phases = 2 * steps + 2 * GROUPS
    ny, nx, nz, nc = torus(groups, members)
    return pl.pallas_call(
        functools.partial(kernel, groups, members, hots),
        out_shape=jax.ShapeDtypeStruct((rows, units), BF16),
        in_specs=[ANY, SCALARS] + [ANY] * 6,
        out_specs=WHOLE,
        scratch_shapes=[
            pltpu.SMEM(ids.shape, jnp.int32),
            VMEM((vocab, width), BF16),
            VMEM((vocab, width), F32),
            VMEM((chunk, width), F32),
            VMEM((CHUNKS, groups, chunk, width), BF16),
            [VMEM((groups, chunk, width), BF16) for _ in range(CHUNKS)],
            VMEM((CHUNKS, members, chunk, cols), BF16),
            VMEM((rows, cols), BF16),
            VMEM((2, depth, units), BF16),
            VMEM((2, max(ny, nx), nz, depth, units), BF16),
            VMEM((ny, nx, nz, nc, 2, depth, units), BF16),
            VMEM(down.shape, BF16),
            VMEM(up.shape, BF16),
            VMEM(bias.shape, F32),
            VMEM(tower_bias.shape, F32),
            VMEM((steps, members, share, rank), BF16),
            VMEM((steps, members - 1, share, rank), BF16),
            VMEM((steps, members, share, rank), BF16),
            VMEM((rows, cols), BF16),
            VMEM((rows, units), F32),
            VMEM((2, height, units), F32),
            VMEM((GROUPS, height, units), BF16),
            VMEM((GROUPS, 2, height // 2, units), BF16),
            VMEM((GROUPS, 2, height, units), BF16),
            VMEM((GROUPS, 2, height, units), BF16),
            DMA((2 * layers + 5,)),
            DMA((CHUNKS,)),
            DMA((CHUNKS,)),
            DMA((CHUNKS, members - 1)),
            DMA((CHUNKS, members - 1)),
            DMA((phases, members - 1)),
            DMA((phases, members - 1)),
            DMA((20,)),
            DMA((20,)),
        ],
        compiler_params=pltpu.CompilerParams(
            collective_id=0, has_side_effects=True, vmem_limit_bytes=56 * 1024 * 1024
        ),
        name="whole",
    )(ids, order, table, weight, down, up, bias, tower_bias)


def body(groups, members, feature_ids, tables, table_of_feature, cross_down, cross_up, cross_bias, tower_weight, tower_bias):
    m = lax.axis_index("mp")
    _, batch, hots = feature_ids.shape
    rows = batch // (groups * members)
    parts = max(1, LANES // rows)
    tiles = jnp.transpose(jnp.transpose(feature_ids[0]).reshape(hots, batch // LANES, LANES), (1, 0, 2))
    tiles = tiles.reshape(groups, members // parts, hots, LANES)
    own_ids = lax.dynamic_index_in_dim(tiles, m // parts, 1, keepdims=False).reshape(-1)
    depth, units = tower_weight.shape
    weight = tower_weight.reshape(2, depth // 2, units)
    return whole(
        own_ids, table_of_feature, tables[0], weight, cross_down, cross_up, cross_bias,
        tower_bias.reshape(1, -1), groups, members, hots, rows,
    )


def solution(mesh):
    groups, members = mesh.shape["dp"], mesh.shape["mp"]
    return jax.shard_map(
        functools.partial(body, groups, members),
        mesh=mesh,
        in_specs=(
            P("dp", None, None),
            P("dp", None, None),
            P(),
            P(None, "mp", None),
            P(None, "mp", None),
            P(None, "mp"),
            P("dp", "mp"),
            P("mp"),
        ),
        out_specs=P("dp", "mp"),
        check_vma=False,
    )
```

```python
import functools

import jax
import jax.numpy as jnp
from jax import lax
from jax.experimental import pallas as pl
from jax.experimental.pallas import tpu as pltpu
from jax.sharding import PartitionSpec as P

MESH = pl.DeviceIdType.MESH
VMEM = pltpu.VMEM
DMA = pltpu.SemaphoreType.DMA
F32 = jnp.float32
BF16 = jnp.bfloat16
WHOLE = pl.BlockSpec(memory_space=pltpu.VMEM)
SCALARS = pl.BlockSpec(memory_space=pltpu.SMEM)
ANY = pl.BlockSpec(memory_space=pl.ANY)
LANES = 128
CHUNKS = 4
GROUPS = 2


def torus(groups, members):
    rest = groups // members
    across = min(4, rest)
    rest //= across
    below = min(2, rest)
    return members, across, below, rest // below


def place(sizes, d):
    _, nx, nz, nc = sizes
    return d // (nx * nz * nc), lax.rem(d // (nz * nc), nx), lax.rem(d // nc, nz), lax.rem(d, nc)


def index_of(sizes, y, x, z, c):
    _, nx, nz, nc = sizes
    return ((y * nx + x) * nz + z) * nc + c


def signal(device):
    pl.semaphore_signal(pltpu.get_barrier_semaphore(), inc=1, device_id=device, device_id_type=MESH)


def remote(src, dst, send, recv, device):
    return pltpu.make_async_remote_copy(
        src_ref=src, dst_ref=dst, send_sem=send, recv_sem=recv, device_id=device, device_id_type=MESH
    )


def kernel(
    groups, members, hots, ids_hbm, order_ref, table_hbm, weight_hbm, down_hbm, up_hbm, bias_hbm, tower_bias_hbm,
    out_ref, ids_ref, table_ref, wide, acc, pooled, recv, packed, emb_ref, mine, quarter_ref, tower_ref,
    down_ref, up_ref, bias_ref, tower_bias_ref, part, arrived, proj, crossed, sums, near_units, far_units, far_in, partial_units, units_in,
    load_sem, dp_send, dp_recv, mp_send, mp_recv, send_sem, recv_sem, w_send, w_recv,
):
    d = lax.axis_index("dp")
    m = lax.axis_index("mp")
    vocab, width = table_ref.shape
    chunk = pooled.shape[2]
    per = groups // members
    rows, cols = emb_ref.shape
    layers, _, rank = down_ref.shape
    height = rows // GROUPS
    share = height // members
    units = out_ref.shape[1]
    sizes = torus(groups, members)
    ny, nx, nz, nc = sizes
    y, x, z, c = place(sizes, d)

    def start(copies):
        for copy in copies:
            copy.start()

    def wait(copies):
        for copy in copies:
            copy.wait()

    pairs = [(ids_hbm, ids_ref), (table_hbm, table_ref), (bias_hbm, bias_ref), (tower_bias_hbm, tower_bias_ref)]
    for layer in range(layers):
        pairs.append((down_hbm.at[layer], down_ref.at[layer]))
        pairs.append((up_hbm.at[layer], up_ref.at[layer]))
    loads = [pltpu.make_async_copy(a, b, load_sem.at[i]) for i, (a, b) in enumerate(pairs)]
    own_weight = pltpu.make_async_copy(weight_hbm, mine, load_sem.at[len(pairs)])
    start(loads[:2])

    def dp_at(k):
        return (lax.rem(d + k, groups), m)

    def mp_at(k):
        return (d, lax.rem(m + k, members))

    turned = (m * per + lax.rem(d, per), d // per)
    moved = d // per != m
    for count, device in ((groups, dp_at), (members, mp_at)):

        def greet(k, carry, device=device):
            signal(device(k))
            return carry

        lax.fori_loop(1, count, greet, 0)

    @pl.when(moved)
    def _():
        signal(turned)

    loads[1].wait()
    step = 256

    def widen(i, carry):
        at = pl.ds(pl.multiple_of(i * step, step), step)
        wide[at, :] = table_ref[at, :].astype(F32)
        return carry

    lax.fori_loop(0, vocab // step, widen, 0)
    loads[0].wait()

    local = CHUNKS * chunk
    parts_in_tile = LANES // local if local < LANES else 1
    lane0 = lax.rem(m, parts_in_tile) * local
    span = hots * LANES

    def lookups(ch, g):
        base = g * span + lane0

        def row(h, j):
            skipped = h * LANES + ch * chunk + j
            return wide[pl.ds(ids_ref.at[pl.ds(skipped, ids_ref.shape[0] - skipped)][base], 1), :]

        for j in range(chunk):
            total = row(0, j)
            for h in range(1, hots):
                total = total + row(h, j)
            acc[j : j + 1, :] = total

    def target(k):
        if nz == 1:
            return lax.rem(d + k, groups)
        flat = groups // nz
        across = 1 - (k - 1) // flat
        u = lax.rem(k - 1, flat) + 1 - across
        return index_of(
            sizes, lax.rem(y + u // (nx * nc), ny), lax.rem(x + lax.rem(u // nc, nx), nx),
            lax.rem(z + across, nz), lax.rem(c + lax.rem(u, nc), nc),
        )

    def dp_copy(ch, g):
        return remote(pooled.at[ch, g], recv[ch].at[d], dp_send.at[ch], dp_recv.at[ch], (g, m))

    def every(ch):
        some = pl.ds(0, groups - 1)
        return remote(pooled.at[ch, some], recv[ch].at[some], dp_send.at[ch], dp_recv.at[ch], dp_at(1))

    def first_block(ch):
        g = target(jnp.int32(1))
        lookups(ch, g)
        return g

    def blocks(ch, low, high, before, send=True):
        def block(k, before):
            pooled[ch, before] = acc[...].astype(BF16)
            now = target(k)
            lookups(ch, now)
            if send:
                dp_copy(ch, before).start()
            return now

        return lax.fori_loop(low, high, block, before)

    def last_block(ch, before):
        pooled[ch, before] = acc[...].astype(BF16)
        lookups(ch, d)
        dp_copy(ch, before).start()
        recv[ch][d] = acc[...].astype(BF16)

    def emb_rows(ch, member):
        return pl.ds(pl.multiple_of((ch * members + member) * chunk, chunk), chunk)

    def mp_copy(ch, k):
        to = lax.rem(m + k, members)
        return remote(
            packed.at[ch, to], emb_ref.at[emb_rows(ch, m)], mp_send.at[ch, k - 1], mp_recv.at[ch, k - 1], mp_at(k)
        )

    def spread(ch):
        every(ch).wait_recv()
        for p in range(groups):
            packed[ch, p // per, :, (p % per) * width : (p % per + 1) * width] = recv[ch][order_ref[p]]
        for k in range(1, members):
            mp_copy(ch, k).start()
        emb_ref[emb_rows(ch, m), :] = packed[ch, m]

    swap = remote(weight_hbm, mine, w_send.at[0], w_recv.at[0], turned)
    right, left = lax.rem(x + 1, nx), lax.rem(x + nx - 1, nx)
    upper, lower = lax.rem(y + 1, ny), lax.rem(y + ny - 1, ny)
    depth = mine.shape[1]
    first, second = pl.ds(0, depth // 2), pl.ds(depth // 2, depth // 2)

    def at(y, x, z, c):
        return (index_of(sizes, y, x, z, c), m)

    to_right, to_left = at(y, right, z, c), at(y, left, z, c)
    to_upper, to_lower = at(upper, x, z, c), at(lower, x, z, c)

    def send_all(number, moves):
        return [
            remote(src, dst, w_send.at[number + i], w_recv.at[number + i], device)
            for i, (src, dst, device) in enumerate(moves)
        ]

    def below():
        if nz == 1:
            return []
        to = at(y, x, 1 - z, c)
        return send_all(1, [(mine.at[0], quarter_ref.at[0, x, z], to), (mine.at[1], quarter_ref.at[1, y, z], to)])

    def beside():
        own = quarter_ref.at[1, y]
        moves = [(own, own, to_upper), (own, own, to_lower)]
        if nx > 1:
            own = quarter_ref.at[0, x]
            moves += [(own, own, to_right), (own, own, to_left)]
        return send_all(3, moves)

    def relayed():
        a, b = quarter_ref.at[1, lower, :, first], quarter_ref.at[1, upper, :, second]
        moves = [(a, a, to_upper), (b, b, to_lower)]
        if nx > 1:
            a, b = quarter_ref.at[0, left, :, first], quarter_ref.at[0, right, :, second]
            moves += [(a, a, to_right), (b, b, to_left)]
        return send_all(7, moves)

    def first_way():
        src, to = quarter_ref.at[0, pl.ds(0, nx)], tower_ref.at[y, :, :, c, 0]
        moves = [(src, to, to_upper), (src, to, to_lower)]
        if nx > 1:
            src, to = quarter_ref.at[1, pl.ds(0, ny)], tower_ref.at[:, x, :, c, 1]
            moves += [(src, to, to_right), (src, to, to_left)]
        return send_all(11, moves)

    def second_way():
        a, b = tower_ref.at[lower, :, :, c, 0, first], tower_ref.at[upper, :, :, c, 0, second]
        moves = [(a, a, to_upper), (b, b, to_lower)]
        if nx > 1:
            a, b = tower_ref.at[:, left, :, c, 1, first], tower_ref.at[:, right, :, c, 1, second]
            moves += [(a, a, to_right), (b, b, to_left)]
        return send_all(15, moves)

    def pair():
        if nc == 1:
            return []
        both = tower_ref.at[:, :, :, c]
        return send_all(19, [(both, both, at(y, x, z, 1 - c))])

    def rows_of(g):
        return pl.ds(g * height, height)

    def scatter(layer, g):
        i = layer * GROUPS + g
        return [
            remote(
                part.at[i, lax.rem(m + k, members)],
                arrived.at[i, k - 1],
                send_sem.at[2 * i, k - 1],
                recv_sem.at[2 * i, k - 1],
                mp_at(k),
            )
            for k in range(1, members)
        ]

    def gather(layer, g):
        i = layer * GROUPS + g
        return [
            remote(
                proj.at[i, m], proj.at[i, m], send_sem.at[2 * i + 1, k - 1], recv_sem.at[2 * i + 1, k - 1], mp_at(k)
            )
            for k in range(1, members)
        ]

    def project(layer, g):
        source = emb_ref if layer == 0 else crossed
        product = jnp.dot(source[rows_of(g), :], down_ref[layer], preferred_element_type=F32)
        i = layer * GROUPS + g
        part[i] = product.astype(BF16).reshape(members, share, rank)
        start(scatter(layer, g))

    def add_up(layer, g):
        i = layer * GROUPS + g
        wait(scatter(layer, g))
        total = part[i, m].astype(F32)
        for k in range(1, members):
            total = total + arrived[i, k - 1].astype(F32)
        proj[i, m] = total.astype(BF16)
        start(gather(layer, g))

    tile = min(512, cols)

    def lift(layer, g):
        i = layer * GROUPS + g
        wait(gather(layer, g))
        source = emb_ref if layer == 0 else crossed
        projected = proj[i].reshape(height, rank)
        here = rows_of(g)

        def columns(j, carry):
            at = pl.ds(pl.multiple_of(j * tile, tile), tile)
            lifted = lax.dot_general(
                projected, up_ref[layer, at, :], (((1,), (1,)), ((), ())), preferred_element_type=F32
            )
            value = emb_ref[here, at].astype(F32) * (lifted + bias_ref[layer : layer + 1, at])
            crossed[here, at] = (value + source[here, at].astype(F32)).astype(BF16)
            return carry

        lax.fori_loop(0, cols // tile, columns, 0)

    def tower(g, block):
        weights = tower_ref[block].reshape(cols, units)
        return jnp.dot(crossed[rows_of(g), :], weights, preferred_element_type=F32)

    tower_phase = 2 * layers * GROUPS
    top, low = pl.ds(0, height // 2), pl.ds(height // 2, height // 2)

    def opposite(g):
        i = tower_phase + 2 * g
        return [
            remote(far_units.at[g, top], far_in.at[g, 0], send_sem.at[i, 0], recv_sem.at[i, 0], mp_at(1)),
            remote(far_units.at[g, low], far_in.at[g, 1], send_sem.at[i, 1], recv_sem.at[i, 1], mp_at(members - 1)),
        ]

    def neighbours(g):
        i = tower_phase + 2 * g + 1
        return [
            remote(partial_units.at[g, 0], units_in.at[g, 0], send_sem.at[i, 0], recv_sem.at[i, 0], mp_at(1)),
            remote(partial_units.at[g, 1], units_in.at[g, 1], send_sem.at[i, 1], recv_sem.at[i, 1], mp_at(members - 1)),
        ]

    def send_far(g):
        far_units[g] = tower(g, lax.rem(m + 2, members)).astype(BF16)
        start(opposite(g))

    def send_near(g):
        for side, k in enumerate((1, members - 1)):
            near_units[side] = tower(g, lax.rem(m + k, members))
        wait(opposite(g))
        partial_units[g, 0, top, :] = (near_units[0, top, :] + far_in[g, 0].astype(F32)).astype(BF16)
        partial_units[g, 0, low, :] = near_units[0, low, :].astype(BF16)
        partial_units[g, 1, top, :] = near_units[1, top, :].astype(BF16)
        partial_units[g, 1, low, :] = (near_units[1, low, :] + far_in[g, 1].astype(F32)).astype(BF16)
        start(neighbours(g))

    in_group = CHUNKS // GROUPS

    def project_first(g):
        for ch in range(g * in_group, (g + 1) * in_group):
            for k in range(1, members):
                mp_copy(ch, k).wait_recv()
        project(0, g)

    cuts = [2, 2 + groups // 4, 1 + groups // 2, 1 + 3 * groups // 4, groups]

    before = blocks(0, cuts[0], cuts[2], first_block(0), send=False)
    pl.semaphore_wait(
        pltpu.get_barrier_semaphore(), groups + members - 2 + jnp.where(moved, 1, 0).astype(jnp.int32)
    )

    def send_first(k, carry):
        dp_copy(0, target(k)).start()
        return carry

    lax.fori_loop(1, cuts[2] - 1, send_first, 0)

    @pl.when(moved)
    def _():
        swap.start()

    @pl.when(jnp.logical_not(moved))
    def _():
        own_weight.start()

    last_block(0, blocks(0, cuts[2], cuts[4], before))
    start(loads[2:])

    @pl.when(moved)
    def _():
        swap.wait()

    @pl.when(jnp.logical_not(moved))
    def _():
        own_weight.wait()

    start(below())
    quarter_ref[0, x, z] = mine[0]
    quarter_ref[1, y, z] = mine[1]
    for ch in range(1, CHUNKS):
        before = blocks(ch, cuts[0], cuts[3], first_block(ch))
        spread(ch - 1)
        last_block(ch, blocks(ch, cuts[3], cuts[4], before))
        if ch == 1:
            wait(below())
            start(beside())
        if ch == 2:
            wait(beside())
            start(relayed())
    for load in loads[2:]:
        load.wait()
    project_first(0)
    spread(CHUNKS - 1)
    wait(relayed())
    start(first_way())
    tower_ref[y, :, :, c, 0] = quarter_ref[0, :nx]
    tower_ref[:, x, :, c, 1] = quarter_ref[1, :ny]
    add_up(0, 0)
    for g in range(1, GROUPS):
        project_first(g)
        add_up(0, g)
    wait(first_way())
    start(second_way())
    for layer in range(1, layers):
        for g in range(GROUPS):
            lift(layer - 1, g)
            project(layer, g)
        if layer == 1:
            wait(second_way())
            start(pair())
        for g in range(GROUPS):
            add_up(layer, g)
    for g in range(GROUPS):
        lift(layers - 1, g)
        if g == 0:
            wait(pair())
        send_far(g)
    for g in range(GROUPS):
        send_near(g)
    for g in range(GROUPS):
        sums[rows_of(g), :] = tower(g, m) + tower_bias_ref[...]
    for g in range(GROUPS):
        wait(neighbours(g))
        total = sums[rows_of(g), :] + units_in[g, 0].astype(F32) + units_in[g, 1].astype(F32)
        total = jnp.maximum(total, 0.0).astype(BF16)
        for ch in range(in_group):
            for member in range(members):
                to = (member * CHUNKS + g * in_group + ch) * chunk
                at0 = (ch * members + member) * chunk
                out_ref[to : to + chunk, :] = total[at0 : at0 + chunk, :]
    for ch in range(CHUNKS):
        every(ch).wait_send()
        for k in range(1, members):
            mp_copy(ch, k).wait_send()


def whole(ids, order, table, weight, down, up, bias, tower_bias, groups, members, hots, local):
    vocab, width = table.shape
    per = groups // members
    chunk = local // CHUNKS
    rows, cols = members * local, per * width
    layers, _, rank = down.shape
    depth, units = weight.shape[1:]
    height = rows // GROUPS
    share = height // members
    steps = layers * GROUPS
    phases = 2 * steps + 2 * GROUPS
    ny, nx, nz, nc = torus(groups, members)
    return pl.pallas_call(
        functools.partial(kernel, groups, members, hots),
        out_shape=jax.ShapeDtypeStruct((rows, units), BF16),
        in_specs=[ANY, SCALARS] + [ANY] * 6,
        out_specs=WHOLE,
        scratch_shapes=[
            pltpu.SMEM(ids.shape, jnp.int32),
            VMEM((vocab, width), BF16),
            VMEM((vocab, width), F32),
            VMEM((chunk, width), F32),
            VMEM((CHUNKS, groups, chunk, width), BF16),
            [VMEM((groups, chunk, width), BF16) for _ in range(CHUNKS)],
            VMEM((CHUNKS, members, chunk, cols), BF16),
            VMEM((rows, cols), BF16),
            VMEM((2, depth, units), BF16),
            VMEM((2, max(ny, nx), nz, depth, units), BF16),
            VMEM((ny, nx, nz, nc, 2, depth, units), BF16),
            VMEM(down.shape, BF16),
            VMEM(up.shape, BF16),
            VMEM(bias.shape, F32),
            VMEM(tower_bias.shape, F32),
            VMEM((steps, members, share, rank), BF16),
            VMEM((steps, members - 1, share, rank), BF16),
            VMEM((steps, members, share, rank), BF16),
            VMEM((rows, cols), BF16),
            VMEM((rows, units), F32),
            VMEM((2, height, units), F32),
            VMEM((GROUPS, height, units), BF16),
            VMEM((GROUPS, 2, height // 2, units), BF16),
            VMEM((GROUPS, 2, height, units), BF16),
            VMEM((GROUPS, 2, height, units), BF16),
            DMA((2 * layers + 5,)),
            DMA((CHUNKS,)),
            DMA((CHUNKS,)),
            DMA((CHUNKS, members - 1)),
            DMA((CHUNKS, members - 1)),
            DMA((phases, members - 1)),
            DMA((phases, members - 1)),
            DMA((20,)),
            DMA((20,)),
        ],
        compiler_params=pltpu.CompilerParams(
            collective_id=0, has_side_effects=True, vmem_limit_bytes=56 * 1024 * 1024
        ),
        name="whole",
    )(ids, order, table, weight, down, up, bias, tower_bias)


def body(groups, members, feature_ids, tables, table_of_feature, cross_down, cross_up, cross_bias, tower_weight, tower_bias):
    m = lax.axis_index("mp")
    _, batch, hots = feature_ids.shape
    rows = batch // (groups * members)
    parts = max(1, LANES // rows)
    tiles = jnp.transpose(jnp.transpose(feature_ids[0]).reshape(hots, batch // LANES, LANES), (1, 0, 2))
    tiles = tiles.reshape(groups, members // parts, hots, LANES)
    own_ids = lax.dynamic_index_in_dim(tiles, m // parts, 1, keepdims=False).reshape(-1)
    depth, units = tower_weight.shape
    weight = tower_weight.reshape(2, depth // 2, units)
    return whole(
        own_ids, table_of_feature, tables[0], weight, cross_down, cross_up, cross_bias,
        tower_bias.reshape(1, -1), groups, members, hots, rows,
    )


def solution(mesh):
    groups, members = mesh.shape["dp"], mesh.shape["mp"]
    return jax.shard_map(
        functools.partial(body, groups, members),
        mesh=mesh,
        in_specs=(
            P("dp", None, None),
            P("dp", None, None),
            P(),
            P(None, "mp", None),
            P(None, "mp", None),
            P(None, "mp"),
            P("dp", "mp"),
            P("mp"),
        ),
        out_specs=P("dp", "mp"),
        check_vma=False,
    )
```

```python
import functools

import jax
import jax.numpy as jnp
from jax import lax
from jax.experimental import pallas as pl
from jax.experimental.pallas import tpu as pltpu
from jax.sharding import PartitionSpec as P

MESH = pl.DeviceIdType.MESH
VMEM = pltpu.VMEM
DMA = pltpu.SemaphoreType.DMA
F32 = jnp.float32
BF16 = jnp.bfloat16
WHOLE = pl.BlockSpec(memory_space=pltpu.VMEM)
SCALARS = pl.BlockSpec(memory_space=pltpu.SMEM)
ANY = pl.BlockSpec(memory_space=pl.ANY)
LANES = 128
CHUNKS = 4
GROUPS = 2


def torus(groups, members):
    rest = groups // members
    across = min(4, rest)
    rest //= across
    below = min(2, rest)
    return members, across, below, rest // below


def place(sizes, d):
    _, nx, nz, nc = sizes
    return d // (nx * nz * nc), lax.rem(d // (nz * nc), nx), lax.rem(d // nc, nz), lax.rem(d, nc)


def index_of(sizes, y, x, z, c):
    _, nx, nz, nc = sizes
    return ((y * nx + x) * nz + z) * nc + c


def signal(device):
    pl.semaphore_signal(pltpu.get_barrier_semaphore(), inc=1, device_id=device, device_id_type=MESH)


def remote(src, dst, send, recv, device):
    return pltpu.make_async_remote_copy(
        src_ref=src, dst_ref=dst, send_sem=send, recv_sem=recv, device_id=device, device_id_type=MESH
    )


def kernel(
    groups, members, hots, ids_hbm, order_ref, table_hbm, weight_hbm, down_hbm, up_hbm, bias_hbm, tower_bias_hbm,
    out_ref, ids_ref, table_ref, wide, acc, pooled, recv, packed, emb_ref, mine, quarter_ref, tower_ref,
    down_ref, up_ref, bias_ref, tower_bias_ref, part, arrived, proj, crossed, sums, near_units, far_units, far_in, partial_units, units_in,
    load_sem, dp_send, dp_recv, mp_send, mp_recv, send_sem, recv_sem, w_send, w_recv,
):
    d = lax.axis_index("dp")
    m = lax.axis_index("mp")
    vocab, width = table_ref.shape
    chunk = pooled.shape[2]
    per = groups // members
    rows, cols = emb_ref.shape
    layers, _, rank = down_ref.shape
    height = rows // GROUPS
    share = height // members
    units = out_ref.shape[1]
    sizes = torus(groups, members)
    ny, nx, nz, nc = sizes
    y, x, z, c = place(sizes, d)

    far_first = sorted(range(1, members), key=lambda k: -min(k, members - k))

    def start(copies):
        for copy in copies:
            copy.start()

    def wait(copies):
        for copy in copies:
            copy.wait()

    pairs = [(ids_hbm, ids_ref), (table_hbm, table_ref), (bias_hbm, bias_ref), (tower_bias_hbm, tower_bias_ref)]
    for layer in range(layers):
        pairs.append((down_hbm.at[layer], down_ref.at[layer]))
        pairs.append((up_hbm.at[layer], up_ref.at[layer]))
    loads = [pltpu.make_async_copy(a, b, load_sem.at[i]) for i, (a, b) in enumerate(pairs)]
    own_weight = pltpu.make_async_copy(weight_hbm, mine, load_sem.at[len(pairs)])
    start(loads[:2])

    def dp_at(k):
        return (lax.rem(d + k, groups), m)

    def mp_at(k):
        return (d, lax.rem(m + k, members))

    turned = (m * per + lax.rem(d, per), d // per)
    moved = d // per != m
    for count, device in ((groups, dp_at), (members, mp_at)):

        def greet(k, carry, device=device):
            signal(device(k))
            return carry

        lax.fori_loop(1, count, greet, 0)

    @pl.when(moved)
    def _():
        signal(turned)

    loads[1].wait()
    step = 256

    def widen(i, carry):
        at = pl.ds(pl.multiple_of(i * step, step), step)
        wide[at, :] = table_ref[at, :].astype(F32)
        return carry

    lax.fori_loop(0, vocab // step, widen, 0)
    loads[0].wait()

    local = CHUNKS * chunk
    parts_in_tile = LANES // local if local < LANES else 1
    lane0 = lax.rem(m, parts_in_tile) * local
    span = hots * LANES

    def lookups(ch, g):
        base = g * span + lane0

        def row(h, j):
            skipped = h * LANES + ch * chunk + j
            return wide[pl.ds(ids_ref.at[pl.ds(skipped, ids_ref.shape[0] - skipped)][base], 1), :]

        for j in range(chunk):
            total = row(0, j)
            for h in range(1, hots):
                total = total + row(h, j)
            acc[j : j + 1, :] = total

    def target(k):
        if nz == 1:
            return lax.rem(d + k, groups)
        flat = groups // nz
        across = 1 - (k - 1) // flat
        u = lax.rem(k - 1, flat) + 1 - across
        return index_of(
            sizes, lax.rem(y + u // (nx * nc), ny), lax.rem(x + lax.rem(u // nc, nx), nx),
            lax.rem(z + across, nz), lax.rem(c + lax.rem(u, nc), nc),
        )

    def dp_copy(ch, g):
        return remote(pooled.at[ch, g], recv[ch].at[d], dp_send.at[ch], dp_recv.at[ch], (g, m))

    def every(ch):
        some = pl.ds(0, groups - 1)
        return remote(pooled.at[ch, some], recv[ch].at[some], dp_send.at[ch], dp_recv.at[ch], dp_at(1))

    def first_block(ch):
        g = target(jnp.int32(1))
        lookups(ch, g)
        return g

    def blocks(ch, low, high, before, send=True):
        def block(k, before):
            pooled[ch, before] = acc[...].astype(BF16)
            now = target(k)
            lookups(ch, now)
            if send:
                dp_copy(ch, before).start()
            return now

        return lax.fori_loop(low, high, block, before)

    def last_block(ch, before):
        pooled[ch, before] = acc[...].astype(BF16)
        lookups(ch, d)
        dp_copy(ch, before).start()
        recv[ch][d] = acc[...].astype(BF16)

    def emb_rows(ch, member):
        return pl.ds(pl.multiple_of((ch * members + member) * chunk, chunk), chunk)

    def mp_copy(ch, k):
        to = lax.rem(m + k, members)
        return remote(
            packed.at[ch, to], emb_ref.at[emb_rows(ch, m)], mp_send.at[ch, k - 1], mp_recv.at[ch, k - 1], mp_at(k)
        )

    def spread(ch):
        every(ch).wait_recv()
        for p in range(groups):
            packed[ch, p // per, :, (p % per) * width : (p % per + 1) * width] = recv[ch][order_ref[p]]
        for k in far_first:
            mp_copy(ch, k).start()
        emb_ref[emb_rows(ch, m), :] = packed[ch, m]

    swap = remote(weight_hbm, mine, w_send.at[0], w_recv.at[0], turned)
    right, left = lax.rem(x + 1, nx), lax.rem(x + nx - 1, nx)
    upper, lower = lax.rem(y + 1, ny), lax.rem(y + ny - 1, ny)
    depth = mine.shape[1]
    first, second = pl.ds(0, depth // 2), pl.ds(depth // 2, depth // 2)

    def at(y, x, z, c):
        return (index_of(sizes, y, x, z, c), m)

    to_right, to_left = at(y, right, z, c), at(y, left, z, c)
    to_upper, to_lower = at(upper, x, z, c), at(lower, x, z, c)

    def send_all(number, moves):
        return [
            remote(src, dst, w_send.at[number + i], w_recv.at[number + i], device)
            for i, (src, dst, device) in enumerate(moves)
        ]

    def below():
        if nz == 1:
            return []
        to = at(y, x, 1 - z, c)
        return send_all(1, [(mine.at[0], quarter_ref.at[0, x, z], to), (mine.at[1], quarter_ref.at[1, y, z], to)])

    def beside():
        own = quarter_ref.at[1, y]
        moves = [(own, own, to_upper), (own, own, to_lower)]
        if nx > 1:
            own = quarter_ref.at[0, x]
            moves += [(own, own, to_right), (own, own, to_left)]
        return send_all(3, moves)

    def relayed():
        a, b = quarter_ref.at[1, lower, :, first], quarter_ref.at[1, upper, :, second]
        moves = [(a, a, to_upper), (b, b, to_lower)]
        if nx > 1:
            a, b = quarter_ref.at[0, left, :, first], quarter_ref.at[0, right, :, second]
            moves += [(a, a, to_right), (b, b, to_left)]
        return send_all(7, moves)

    def first_way():
        src, to = quarter_ref.at[0, pl.ds(0, nx)], tower_ref.at[y, :, :, c, 0]
        moves = [(src, to, to_upper), (src, to, to_lower)]
        if nx > 1:
            src, to = quarter_ref.at[1, pl.ds(0, ny)], tower_ref.at[:, x, :, c, 1]
            moves += [(src, to, to_right), (src, to, to_left)]
        return send_all(11, moves)

    def second_way():
        a, b = tower_ref.at[lower, :, :, c, 0, first], tower_ref.at[upper, :, :, c, 0, second]
        moves = [(a, a, to_upper), (b, b, to_lower)]
        if nx > 1:
            a, b = tower_ref.at[:, left, :, c, 1, first], tower_ref.at[:, right, :, c, 1, second]
            moves += [(a, a, to_right), (b, b, to_left)]
        return send_all(15, moves)

    def pair():
        if nc == 1:
            return []
        both = tower_ref.at[:, :, :, c]
        return send_all(19, [(both, both, at(y, x, z, 1 - c))])

    def rows_of(g):
        return pl.ds(g * height, height)

    def scatter(layer, g):
        i = layer * GROUPS + g
        return [
            remote(
                part.at[i, lax.rem(m + k, members)],
                arrived.at[i, k - 1],
                send_sem.at[2 * i, k - 1],
                recv_sem.at[2 * i, k - 1],
                mp_at(k),
            )
            for k in far_first
        ]

    def gather(layer, g):
        i = layer * GROUPS + g
        return [
            remote(
                proj.at[i, m], proj.at[i, m], send_sem.at[2 * i + 1, k - 1], recv_sem.at[2 * i + 1, k - 1], mp_at(k)
            )
            for k in far_first
        ]

    def project(layer, g):
        source = emb_ref if layer == 0 else crossed
        product = jnp.dot(source[rows_of(g), :], down_ref[layer], preferred_element_type=F32)
        i = layer * GROUPS + g
        part[i] = product.astype(BF16).reshape(members, share, rank)
        start(scatter(layer, g))

    def add_up(layer, g):
        i = layer * GROUPS + g
        wait(scatter(layer, g))
        total = part[i, m].astype(F32)
        for k in range(1, members):
            total = total + arrived[i, k - 1].astype(F32)
        proj[i, m] = total.astype(BF16)
        start(gather(layer, g))

    tile = min(512, cols)

    def lift(layer, g):
        i = layer * GROUPS + g
        wait(gather(layer, g))
        source = emb_ref if layer == 0 else crossed
        projected = proj[i].reshape(height, rank)
        here = rows_of(g)

        def columns(j, carry):
            at = pl.ds(pl.multiple_of(j * tile, tile), tile)
            lifted = lax.dot_general(
                projected, up_ref[layer, at, :], (((1,), (1,)), ((), ())), preferred_element_type=F32
            )
            value = emb_ref[here, at].astype(F32) * (lifted + bias_ref[layer : layer + 1, at])
            crossed[here, at] = (value + source[here, at].astype(F32)).astype(BF16)
            return carry

        lax.fori_loop(0, cols // tile, columns, 0)

    def tower(g, block):
        weights = tower_ref[block].reshape(cols, units)
        return jnp.dot(crossed[rows_of(g), :], weights, preferred_element_type=F32)

    tower_phase = 2 * layers * GROUPS
    top, low = pl.ds(0, height // 2), pl.ds(height // 2, height // 2)

    def opposite(g):
        i = tower_phase + 2 * g
        return [
            remote(far_units.at[g, top], far_in.at[g, 0], send_sem.at[i, 0], recv_sem.at[i, 0], mp_at(1)),
            remote(far_units.at[g, low], far_in.at[g, 1], send_sem.at[i, 1], recv_sem.at[i, 1], mp_at(members - 1)),
        ]

    def neighbours(g):
        i = tower_phase + 2 * g + 1
        return [
            remote(partial_units.at[g, 0], units_in.at[g, 0], send_sem.at[i, 0], recv_sem.at[i, 0], mp_at(1)),
            remote(partial_units.at[g, 1], units_in.at[g, 1], send_sem.at[i, 1], recv_sem.at[i, 1], mp_at(members - 1)),
        ]

    def send_far(g):
        far_units[g] = tower(g, lax.rem(m + 2, members)).astype(BF16)
        start(opposite(g))

    def send_near(g):
        for side, k in enumerate((1, members - 1)):
            near_units[side] = tower(g, lax.rem(m + k, members))
        wait(opposite(g))
        partial_units[g, 0, top, :] = (near_units[0, top, :] + far_in[g, 0].astype(F32)).astype(BF16)
        partial_units[g, 0, low, :] = near_units[0, low, :].astype(BF16)
        partial_units[g, 1, top, :] = near_units[1, top, :].astype(BF16)
        partial_units[g, 1, low, :] = (near_units[1, low, :] + far_in[g, 1].astype(F32)).astype(BF16)
        start(neighbours(g))

    in_group = CHUNKS // GROUPS

    def project_first(g):
        for ch in range(g * in_group, (g + 1) * in_group):
            for k in range(1, members):
                mp_copy(ch, k).wait_recv()
        project(0, g)

    cuts = [2, 2 + groups // 4, 1 + groups // 2, 1 + 3 * groups // 4, groups]

    before = blocks(0, cuts[0], cuts[1], first_block(0), send=False)
    pl.semaphore_wait(
        pltpu.get_barrier_semaphore(), groups + members - 2 + jnp.where(moved, 1, 0).astype(jnp.int32)
    )

    def send_first(k, carry):
        dp_copy(0, target(k)).start()
        return carry

    lax.fori_loop(1, cuts[1] - 1, send_first, 0)

    @pl.when(moved)
    def _():
        swap.start()

    @pl.when(jnp.logical_not(moved))
    def _():
        own_weight.start()

    last_block(0, blocks(0, cuts[1], cuts[4], before))
    start(loads[2:])

    @pl.when(moved)
    def _():
        swap.wait()

    @pl.when(jnp.logical_not(moved))
    def _():
        own_weight.wait()

    start(below())
    quarter_ref[0, x, z] = mine[0]
    quarter_ref[1, y, z] = mine[1]
    for ch in range(1, CHUNKS):
        before = blocks(ch, cuts[0], cuts[3], first_block(ch))
        spread(ch - 1)
        last_block(ch, blocks(ch, cuts[3], cuts[4], before))
        if ch == 1:
            wait(below())
            start(beside())
        if ch == 2:
            wait(beside())
            start(relayed())
    for load in loads[2:]:
        load.wait()
    project_first(0)
    spread(CHUNKS - 1)
    wait(relayed())
    start(first_way())
    tower_ref[y, :, :, c, 0] = quarter_ref[0, :nx]
    tower_ref[:, x, :, c, 1] = quarter_ref[1, :ny]
    add_up(0, 0)
    for g in range(1, GROUPS):
        project_first(g)
        add_up(0, g)
    wait(first_way())
    start(second_way())
    for layer in range(1, layers):
        for g in range(GROUPS):
            lift(layer - 1, g)
            project(layer, g)
        if layer == 1:
            wait(second_way())
            start(pair())
        for g in range(GROUPS):
            add_up(layer, g)
    for g in range(GROUPS):
        lift(layers - 1, g)
        if g == 0:
            wait(pair())
        send_far(g)
    for g in range(GROUPS):
        send_near(g)
    for g in range(GROUPS):
        sums[rows_of(g), :] = tower(g, m) + tower_bias_ref[...]
    for g in range(GROUPS):
        wait(neighbours(g))
        total = sums[rows_of(g), :] + units_in[g, 0].astype(F32) + units_in[g, 1].astype(F32)
        total = jnp.maximum(total, 0.0).astype(BF16)
        for ch in range(in_group):
            for member in range(members):
                to = (member * CHUNKS + g * in_group + ch) * chunk
                at0 = (ch * members + member) * chunk
                out_ref[to : to + chunk, :] = total[at0 : at0 + chunk, :]
    for ch in range(CHUNKS):
        every(ch).wait_send()
        for k in range(1, members):
            mp_copy(ch, k).wait_send()


def whole(ids, order, table, weight, down, up, bias, tower_bias, groups, members, hots, local):
    vocab, width = table.shape
    per = groups // members
    chunk = local // CHUNKS
    rows, cols = members * local, per * width
    layers, _, rank = down.shape
    depth, units = weight.shape[1:]
    height = rows // GROUPS
    share = height // members
    steps = layers * GROUPS
    phases = 2 * steps + 2 * GROUPS
    ny, nx, nz, nc = torus(groups, members)
    return pl.pallas_call(
        functools.partial(kernel, groups, members, hots),
        out_shape=jax.ShapeDtypeStruct((rows, units), BF16),
        in_specs=[ANY, SCALARS] + [ANY] * 6,
        out_specs=WHOLE,
        scratch_shapes=[
            pltpu.SMEM(ids.shape, jnp.int32),
            VMEM((vocab, width), BF16),
            VMEM((vocab, width), F32),
            VMEM((chunk, width), F32),
            VMEM((CHUNKS, groups, chunk, width), BF16),
            [VMEM((groups, chunk, width), BF16) for _ in range(CHUNKS)],
            VMEM((CHUNKS, members, chunk, cols), BF16),
            VMEM((rows, cols), BF16),
            VMEM((2, depth, units), BF16),
            VMEM((2, max(ny, nx), nz, depth, units), BF16),
            VMEM((ny, nx, nz, nc, 2, depth, units), BF16),
            VMEM(down.shape, BF16),
            VMEM(up.shape, BF16),
            VMEM(bias.shape, F32),
            VMEM(tower_bias.shape, F32),
            VMEM((steps, members, share, rank), BF16),
            VMEM((steps, members - 1, share, rank), BF16),
            VMEM((steps, members, share, rank), BF16),
            VMEM((rows, cols), BF16),
            VMEM((rows, units), F32),
            VMEM((2, height, units), F32),
            VMEM((GROUPS, height, units), BF16),
            VMEM((GROUPS, 2, height // 2, units), BF16),
            VMEM((GROUPS, 2, height, units), BF16),
            VMEM((GROUPS, 2, height, units), BF16),
            DMA((2 * layers + 5,)),
            DMA((CHUNKS,)),
            DMA((CHUNKS,)),
            DMA((CHUNKS, members - 1)),
            DMA((CHUNKS, members - 1)),
            DMA((phases, members - 1)),
            DMA((phases, members - 1)),
            DMA((20,)),
            DMA((20,)),
        ],
        compiler_params=pltpu.CompilerParams(
            collective_id=0, has_side_effects=True, vmem_limit_bytes=56 * 1024 * 1024
        ),
        name="whole",
    )(ids, order, table, weight, down, up, bias, tower_bias)


def body(groups, members, feature_ids, tables, table_of_feature, cross_down, cross_up, cross_bias, tower_weight, tower_bias):
    m = lax.axis_index("mp")
    _, batch, hots = feature_ids.shape
    rows = batch // (groups * members)
    parts = max(1, LANES // rows)
    tiles = jnp.transpose(jnp.transpose(feature_ids[0]).reshape(hots, batch // LANES, LANES), (1, 0, 2))
    tiles = tiles.reshape(groups, members // parts, hots, LANES)
    own_ids = lax.dynamic_index_in_dim(tiles, m // parts, 1, keepdims=False).reshape(-1)
    depth, units = tower_weight.shape
    weight = tower_weight.reshape(2, depth // 2, units)
    return whole(
        own_ids, table_of_feature, tables[0], weight, cross_down, cross_up, cross_bias,
        tower_bias.reshape(1, -1), groups, members, hots, rows,
    )


def solution(mesh):
    groups, members = mesh.shape["dp"], mesh.shape["mp"]
    return jax.shard_map(
        functools.partial(body, groups, members),
        mesh=mesh,
        in_specs=(
            P("dp", None, None),
            P("dp", None, None),
            P(),
            P(None, "mp", None),
            P(None, "mp", None),
            P(None, "mp"),
            P("dp", "mp"),
            P("mp"),
        ),
        out_specs=P("dp", "mp"),
        check_vma=False,
    )
```

```python
import functools

import jax
import jax.numpy as jnp
from jax import lax
from jax.experimental import pallas as pl
from jax.experimental.pallas import tpu as pltpu
from jax.sharding import PartitionSpec as P

MESH = pl.DeviceIdType.MESH
VMEM = pltpu.VMEM
DMA = pltpu.SemaphoreType.DMA
F32 = jnp.float32
BF16 = jnp.bfloat16
WHOLE = pl.BlockSpec(memory_space=pltpu.VMEM)
SCALARS = pl.BlockSpec(memory_space=pltpu.SMEM)
ANY = pl.BlockSpec(memory_space=pl.ANY)
LANES = 128
CHUNKS = 4
GROUPS = 2


def torus(groups, members):
    rest = groups // members
    across = min(4, rest)
    rest //= across
    below = min(2, rest)
    return members, across, below, rest // below


def place(sizes, d):
    _, nx, nz, nc = sizes
    return d // (nx * nz * nc), lax.rem(d // (nz * nc), nx), lax.rem(d // nc, nz), lax.rem(d, nc)


def index_of(sizes, y, x, z, c):
    _, nx, nz, nc = sizes
    return ((y * nx + x) * nz + z) * nc + c


def signal(device):
    pl.semaphore_signal(pltpu.get_barrier_semaphore(), inc=1, device_id=device, device_id_type=MESH)


def remote(src, dst, send, recv, device):
    return pltpu.make_async_remote_copy(
        src_ref=src, dst_ref=dst, send_sem=send, recv_sem=recv, device_id=device, device_id_type=MESH
    )


def kernel(
    groups, members, hots, ids_hbm, order_ref, table_hbm, weight_hbm, down_hbm, up_hbm, bias_hbm, tower_bias_hbm,
    out_ref, ids_ref, table_ref, wide, acc, pooled, recv, packed, emb_ref, mine, quarter_ref, tower_ref,
    down_ref, up_ref, bias_ref, tower_bias_ref, part, arrived, proj, crossed, sums, near_units, far_units, far_in, partial_units, units_in,
    load_sem, dp_send, dp_recv, mp_send, mp_recv, send_sem, recv_sem, w_send, w_recv,
):
    d = lax.axis_index("dp")
    m = lax.axis_index("mp")
    vocab, width = table_ref.shape
    chunk = pooled.shape[2]
    per = groups // members
    rows, cols = emb_ref.shape
    layers, _, rank = down_ref.shape
    height = rows // GROUPS
    share = height // members
    units = out_ref.shape[1]
    sizes = torus(groups, members)
    ny, nx, nz, nc = sizes
    y, x, z, c = place(sizes, d)

    far_first = sorted(range(1, members), key=lambda k: -min(k, members - k))

    def start(copies):
        for copy in copies:
            copy.start()

    def wait(copies):
        for copy in copies:
            copy.wait()

    pairs = [(ids_hbm, ids_ref), (table_hbm, table_ref), (bias_hbm, bias_ref), (tower_bias_hbm, tower_bias_ref)]
    for layer in range(layers):
        pairs.append((down_hbm.at[layer], down_ref.at[layer]))
        pairs.append((up_hbm.at[layer], up_ref.at[layer]))
    loads = [pltpu.make_async_copy(a, b, load_sem.at[i]) for i, (a, b) in enumerate(pairs)]
    own_weight = pltpu.make_async_copy(weight_hbm, mine, load_sem.at[len(pairs)])
    start(loads[:2])

    def dp_at(k):
        return (lax.rem(d + k, groups), m)

    def mp_at(k):
        return (d, lax.rem(m + k, members))

    turned = (m * per + lax.rem(d, per), d // per)
    moved = d // per != m
    for count, device in ((groups, dp_at), (members, mp_at)):

        def greet(k, carry, device=device):
            signal(device(k))
            return carry

        lax.fori_loop(1, count, greet, 0)

    @pl.when(moved)
    def _():
        signal(turned)

    loads[1].wait()
    step = 256

    def widen(i, carry):
        at = pl.ds(pl.multiple_of(i * step, step), step)
        wide[at, :] = table_ref[at, :].astype(F32)
        return carry

    lax.fori_loop(0, vocab // step, widen, 0)
    loads[0].wait()

    local = CHUNKS * chunk
    parts_in_tile = LANES // local if local < LANES else 1
    lane0 = lax.rem(m, parts_in_tile) * local
    span = hots * LANES

    def lookups(ch, g):
        base = g * span + lane0

        def row(h, j):
            skipped = h * LANES + ch * chunk + j
            return wide[pl.ds(ids_ref.at[pl.ds(skipped, ids_ref.shape[0] - skipped)][base], 1), :]

        for j in range(chunk):
            total = row(0, j)
            for h in range(1, hots):
                total = total + row(h, j)
            acc[j : j + 1, :] = total

    def target(k):
        if nz == 1:
            return lax.rem(d + k, groups)
        flat = groups // nz
        across = 1 - (k - 1) // flat
        u = lax.rem(k - 1, flat) + 1 - across
        return index_of(
            sizes, lax.rem(y + u // (nx * nc), ny), lax.rem(x + lax.rem(u // nc, nx), nx),
            lax.rem(z + across, nz), lax.rem(c + lax.rem(u, nc), nc),
        )

    def dp_copy(ch, g):
        return remote(pooled.at[ch, g], recv[ch].at[d], dp_send.at[ch], dp_recv.at[ch], (g, m))

    def every(ch):
        some = pl.ds(0, groups - 1)
        return remote(pooled.at[ch, some], recv[ch].at[some], dp_send.at[ch], dp_recv.at[ch], dp_at(1))

    def first_block(ch):
        g = target(jnp.int32(1))
        lookups(ch, g)
        return g

    def blocks(ch, low, high, before, send=True):
        def block(k, before):
            pooled[ch, before] = acc[...].astype(BF16)
            now = target(k)
            lookups(ch, now)
            if send:
                dp_copy(ch, before).start()
            return now

        return lax.fori_loop(low, high, block, before)

    def last_block(ch, before):
        pooled[ch, before] = acc[...].astype(BF16)
        lookups(ch, d)
        dp_copy(ch, before).start()
        recv[ch][d] = acc[...].astype(BF16)

    def emb_rows(ch, member):
        return pl.ds(pl.multiple_of((ch * members + member) * chunk, chunk), chunk)

    def mp_copy(ch, k):
        to = lax.rem(m + k, members)
        return remote(
            packed.at[ch, to], emb_ref.at[emb_rows(ch, m)], mp_send.at[ch, k - 1], mp_recv.at[ch, k - 1], mp_at(k)
        )

    def spread(ch):
        every(ch).wait_recv()
        for p in range(groups):
            packed[ch, p // per, :, (p % per) * width : (p % per + 1) * width] = recv[ch][order_ref[p]]
        for k in far_first:
            mp_copy(ch, k).start()
        emb_ref[emb_rows(ch, m), :] = packed[ch, m]

    swap = remote(weight_hbm, mine, w_send.at[0], w_recv.at[0], turned)
    right, left = lax.rem(x + 1, nx), lax.rem(x + nx - 1, nx)
    upper, lower = lax.rem(y + 1, ny), lax.rem(y + ny - 1, ny)
    depth = mine.shape[1]
    first, second = pl.ds(0, depth // 2), pl.ds(depth // 2, depth // 2)

    def at(y, x, z, c):
        return (index_of(sizes, y, x, z, c), m)

    to_right, to_left = at(y, right, z, c), at(y, left, z, c)
    to_upper, to_lower = at(upper, x, z, c), at(lower, x, z, c)

    def send_all(number, moves):
        return [
            remote(src, dst, w_send.at[number + i], w_recv.at[number + i], device)
            for i, (src, dst, device) in enumerate(moves)
        ]

    def below():
        if nz == 1:
            return []
        to = at(y, x, 1 - z, c)
        return send_all(1, [(mine.at[0], quarter_ref.at[0, x, z], to), (mine.at[1], quarter_ref.at[1, y, z], to)])

    def beside():
        own = quarter_ref.at[1, y]
        moves = [(own, own, to_upper), (own, own, to_lower)]
        if nx > 1:
            own = quarter_ref.at[0, x]
            moves += [(own, own, to_right), (own, own, to_left)]
        return send_all(3, moves)

    def relayed():
        a, b = quarter_ref.at[1, lower, :, first], quarter_ref.at[1, upper, :, second]
        moves = [(a, a, to_upper), (b, b, to_lower)]
        if nx > 1:
            a, b = quarter_ref.at[0, left, :, first], quarter_ref.at[0, right, :, second]
            moves += [(a, a, to_right), (b, b, to_left)]
        return send_all(7, moves)

    def first_way():
        src, to = quarter_ref.at[0, pl.ds(0, nx)], tower_ref.at[y, :, :, c, 0]
        moves = [(src, to, to_upper), (src, to, to_lower)]
        if nx > 1:
            src, to = quarter_ref.at[1, pl.ds(0, ny)], tower_ref.at[:, x, :, c, 1]
            moves += [(src, to, to_right), (src, to, to_left)]
        return send_all(11, moves)

    def second_way():
        a, b = tower_ref.at[lower, :, :, c, 0, first], tower_ref.at[upper, :, :, c, 0, second]
        moves = [(a, a, to_upper), (b, b, to_lower)]
        if nx > 1:
            a, b = tower_ref.at[:, left, :, c, 1, first], tower_ref.at[:, right, :, c, 1, second]
            moves += [(a, a, to_right), (b, b, to_left)]
        return send_all(15, moves)

    def pair():
        if nc == 1:
            return []
        both = tower_ref.at[:, :, :, c]
        return send_all(19, [(both, both, at(y, x, z, 1 - c))])

    def rows_of(g):
        return pl.ds(g * height, height)

    def scatter(layer, g):
        i = layer * GROUPS + g
        return [
            remote(
                part.at[i, lax.rem(m + k, members)],
                arrived.at[i, k - 1],
                send_sem.at[2 * i, k - 1],
                recv_sem.at[2 * i, k - 1],
                mp_at(k),
            )
            for k in far_first
        ]

    def gather(layer, g):
        i = layer * GROUPS + g
        return [
            remote(
                proj.at[i, m], proj.at[i, m], send_sem.at[2 * i + 1, k - 1], recv_sem.at[2 * i + 1, k - 1], mp_at(k)
            )
            for k in far_first
        ]

    def project(layer, g):
        source = emb_ref if layer == 0 else crossed
        product = jnp.dot(source[rows_of(g), :], down_ref[layer], preferred_element_type=F32)
        i = layer * GROUPS + g
        part[i] = product.astype(BF16).reshape(members, share, rank)
        start(scatter(layer, g))

    def add_up(layer, g):
        i = layer * GROUPS + g
        wait(scatter(layer, g))
        total = part[i, m].astype(F32)
        for k in range(1, members):
            total = total + arrived[i, k - 1].astype(F32)
        proj[i, m] = total.astype(BF16)
        start(gather(layer, g))

    tile = min(512, cols)

    def lift(layer, g):
        i = layer * GROUPS + g
        wait(gather(layer, g))
        source = emb_ref if layer == 0 else crossed
        projected = proj[i].reshape(height, rank)
        here = rows_of(g)

        def columns(j, carry):
            at = pl.ds(pl.multiple_of(j * tile, tile), tile)
            lifted = lax.dot_general(
                projected, up_ref[layer, at, :], (((1,), (1,)), ((), ())), preferred_element_type=F32
            )
            value = emb_ref[here, at].astype(F32) * (lifted + bias_ref[layer : layer + 1, at])
            crossed[here, at] = (value + source[here, at].astype(F32)).astype(BF16)
            return carry

        lax.fori_loop(0, cols // tile, columns, 0)

    def tower(g, block):
        weights = tower_ref[block].reshape(cols, units)
        return jnp.dot(crossed[rows_of(g), :], weights, preferred_element_type=F32)

    tower_phase = 2 * layers * GROUPS
    top, low = pl.ds(0, height // 2), pl.ds(height // 2, height // 2)

    def opposite(g):
        i = tower_phase + 2 * g
        return [
            remote(far_units.at[g, top], far_in.at[g, 0], send_sem.at[i, 0], recv_sem.at[i, 0], mp_at(1)),
            remote(far_units.at[g, low], far_in.at[g, 1], send_sem.at[i, 1], recv_sem.at[i, 1], mp_at(members - 1)),
        ]

    def neighbours(g):
        i = tower_phase + 2 * g + 1
        return [
            remote(partial_units.at[g, 0], units_in.at[g, 0], send_sem.at[i, 0], recv_sem.at[i, 0], mp_at(1)),
            remote(partial_units.at[g, 1], units_in.at[g, 1], send_sem.at[i, 1], recv_sem.at[i, 1], mp_at(members - 1)),
        ]

    def send_far(g):
        far_units[g] = tower(g, lax.rem(m + 2, members)).astype(BF16)
        start(opposite(g))

    def send_near(g):
        for side, k in enumerate((1, members - 1)):
            near_units[side] = tower(g, lax.rem(m + k, members))
        wait(opposite(g))
        partial_units[g, 0, top, :] = (near_units[0, top, :] + far_in[g, 0].astype(F32)).astype(BF16)
        partial_units[g, 0, low, :] = near_units[0, low, :].astype(BF16)
        partial_units[g, 1, top, :] = near_units[1, top, :].astype(BF16)
        partial_units[g, 1, low, :] = (near_units[1, low, :] + far_in[g, 1].astype(F32)).astype(BF16)
        start(neighbours(g))

    in_group = CHUNKS // GROUPS

    def project_first(g):
        for ch in range(g * in_group, (g + 1) * in_group):
            for k in range(1, members):
                mp_copy(ch, k).wait_recv()
        project(0, g)

    early = 2 + groups // 16
    cuts = [2, 2 + groups // 4, 1 + groups // 2, 1 + 3 * groups // 4, groups]

    before = blocks(0, cuts[0], early, first_block(0), send=False)
    pl.semaphore_wait(
        pltpu.get_barrier_semaphore(), groups + members - 2 + jnp.where(moved, 1, 0).astype(jnp.int32)
    )

    def send_first(k, carry):
        dp_copy(0, target(k)).start()
        return carry

    lax.fori_loop(1, early - 1, send_first, 0)

    @pl.when(moved)
    def _():
        swap.start()

    @pl.when(jnp.logical_not(moved))
    def _():
        own_weight.start()

    last_block(0, blocks(0, early, cuts[4], before))
    start(loads[2:])

    @pl.when(moved)
    def _():
        swap.wait()

    @pl.when(jnp.logical_not(moved))
    def _():
        own_weight.wait()

    start(below())
    quarter_ref[0, x, z] = mine[0]
    quarter_ref[1, y, z] = mine[1]
    for ch in range(1, CHUNKS):
        before = blocks(ch, cuts[0], cuts[3], first_block(ch))
        spread(ch - 1)
        last_block(ch, blocks(ch, cuts[3], cuts[4], before))
        if ch == 1:
            wait(below())
            start(beside())
        if ch == 2:
            wait(beside())
            start(relayed())
    for load in loads[2:]:
        load.wait()
    project_first(0)
    spread(CHUNKS - 1)
    wait(relayed())
    start(first_way())
    tower_ref[y, :, :, c, 0] = quarter_ref[0, :nx]
    tower_ref[:, x, :, c, 1] = quarter_ref[1, :ny]
    add_up(0, 0)
    for g in range(1, GROUPS):
        project_first(g)
        add_up(0, g)
    wait(first_way())
    start(second_way())
    for layer in range(1, layers):
        for g in range(GROUPS):
            lift(layer - 1, g)
            project(layer, g)
        if layer == 1:
            wait(second_way())
            start(pair())
        for g in range(GROUPS):
            add_up(layer, g)
    for g in range(GROUPS):
        lift(layers - 1, g)
        if g == 0:
            wait(pair())
        send_far(g)
    for g in range(GROUPS):
        send_near(g)
    for g in range(GROUPS):
        sums[rows_of(g), :] = tower(g, m) + tower_bias_ref[...]
    for g in range(GROUPS):
        wait(neighbours(g))
        total = sums[rows_of(g), :] + units_in[g, 0].astype(F32) + units_in[g, 1].astype(F32)
        total = jnp.maximum(total, 0.0).astype(BF16)
        for ch in range(in_group):
            for member in range(members):
                to = (member * CHUNKS + g * in_group + ch) * chunk
                at0 = (ch * members + member) * chunk
                out_ref[to : to + chunk, :] = total[at0 : at0 + chunk, :]
    for ch in range(CHUNKS):
        every(ch).wait_send()
        for k in range(1, members):
            mp_copy(ch, k).wait_send()


def whole(ids, order, table, weight, down, up, bias, tower_bias, groups, members, hots, local):
    vocab, width = table.shape
    per = groups // members
    chunk = local // CHUNKS
    rows, cols = members * local, per * width
    layers, _, rank = down.shape
    depth, units = weight.shape[1:]
    height = rows // GROUPS
    share = height // members
    steps = layers * GROUPS
    phases = 2 * steps + 2 * GROUPS
    ny, nx, nz, nc = torus(groups, members)
    return pl.pallas_call(
        functools.partial(kernel, groups, members, hots),
        out_shape=jax.ShapeDtypeStruct((rows, units), BF16),
        in_specs=[ANY, SCALARS] + [ANY] * 6,
        out_specs=WHOLE,
        scratch_shapes=[
            pltpu.SMEM(ids.shape, jnp.int32),
            VMEM((vocab, width), BF16),
            VMEM((vocab, width), F32),
            VMEM((chunk, width), F32),
            VMEM((CHUNKS, groups, chunk, width), BF16),
            [VMEM((groups, chunk, width), BF16) for _ in range(CHUNKS)],
            VMEM((CHUNKS, members, chunk, cols), BF16),
            VMEM((rows, cols), BF16),
            VMEM((2, depth, units), BF16),
            VMEM((2, max(ny, nx), nz, depth, units), BF16),
            VMEM((ny, nx, nz, nc, 2, depth, units), BF16),
            VMEM(down.shape, BF16),
            VMEM(up.shape, BF16),
            VMEM(bias.shape, F32),
            VMEM(tower_bias.shape, F32),
            VMEM((steps, members, share, rank), BF16),
            VMEM((steps, members - 1, share, rank), BF16),
            VMEM((steps, members, share, rank), BF16),
            VMEM((rows, cols), BF16),
            VMEM((rows, units), F32),
            VMEM((2, height, units), F32),
            VMEM((GROUPS, height, units), BF16),
            VMEM((GROUPS, 2, height // 2, units), BF16),
            VMEM((GROUPS, 2, height, units), BF16),
            VMEM((GROUPS, 2, height, units), BF16),
            DMA((2 * layers + 5,)),
            DMA((CHUNKS,)),
            DMA((CHUNKS,)),
            DMA((CHUNKS, members - 1)),
            DMA((CHUNKS, members - 1)),
            DMA((phases, members - 1)),
            DMA((phases, members - 1)),
            DMA((20,)),
            DMA((20,)),
        ],
        compiler_params=pltpu.CompilerParams(
            collective_id=0, has_side_effects=True, vmem_limit_bytes=56 * 1024 * 1024
        ),
        name="whole",
    )(ids, order, table, weight, down, up, bias, tower_bias)


def body(groups, members, feature_ids, tables, table_of_feature, cross_down, cross_up, cross_bias, tower_weight, tower_bias):
    m = lax.axis_index("mp")
    _, batch, hots = feature_ids.shape
    rows = batch // (groups * members)
    parts = max(1, LANES // rows)
    tiles = jnp.transpose(jnp.transpose(feature_ids[0]).reshape(hots, batch // LANES, LANES), (1, 0, 2))
    tiles = tiles.reshape(groups, members // parts, hots, LANES)
    own_ids = lax.dynamic_index_in_dim(tiles, m // parts, 1, keepdims=False).reshape(-1)
    depth, units = tower_weight.shape
    weight = tower_weight.reshape(2, depth // 2, units)
    return whole(
        own_ids, table_of_feature, tables[0], weight, cross_down, cross_up, cross_bias,
        tower_bias.reshape(1, -1), groups, members, hots, rows,
    )


def solution(mesh):
    groups, members = mesh.shape["dp"], mesh.shape["mp"]
    return jax.shard_map(
        functools.partial(body, groups, members),
        mesh=mesh,
        in_specs=(
            P("dp", None, None),
            P("dp", None, None),
            P(),
            P(None, "mp", None),
            P(None, "mp", None),
            P(None, "mp"),
            P("dp", "mp"),
            P("mp"),
        ),
        out_specs=P("dp", "mp"),
        check_vma=False,
    )
```
